256 devices in a mesh: unit: 4 (over x), north: 4 (over y), east: 16 (over z, core).
Axes of the slice: x: 4, y: 4, z: 8, core: 2. Of those that a mesh axis runs over, the one named last changes fastest.
Arguments:
- pair_rows: bfloat16 [2048, 512, 128], P(('unit', 'north'), 'east'), parts along dimension 0, may hold values from -6 to 6
- in_gain: float32 [128], replicated, may hold values from 0.25 to 1.75
- left_weight: bfloat16 [512, 128], P('unit'), parts along dimension 0, may hold values from -0.5 to 0.5
- right_weight: bfloat16 [512, 128], P('unit'), parts along dimension 0, may hold values from -0.5 to 0.5
- left_gate: bfloat16 [512, 128], P('unit'), parts along dimension 0, may hold values from -0.5 to 0.5
- right_gate: bfloat16 [512, 128], P('unit'), parts along dimension 0, may hold values from -0.5 to 0.5
- mid_gain: float32 [128], replicated, may hold values from 0.25 to 1.75
- out_weight: bfloat16 [512, 128], P('unit'), parts along dimension 0, may hold values from -0.5 to 0.5
- out_gate: bfloat16 [512, 128], P('unit'), parts along dimension 0, may hold values from -0.5 to 0.5
Outputs:
- triangle_out: bfloat16 [2048, 512, 128], P(('unit', 'north'), 'east'), parts along dimension 0
The draws below stay inside these ranges and needn't reach their ends.
There are 4 independent parts, one for each index of `unit`. The reference program is written for one: setup_inputs(seed, part) draws one part's arguments, and reference() takes and returns one part's arrays. A program takes and returns all parts, laid end to end along the dimension named above; an argument that names none is the same for every part. Nothing has to cross between parts.
All inputs are finite; a program needn't handle non-finite values.
Results may differ from the reference program's by a relative error of at most 0.015.
Values may be sent and summed in bfloat16 or wider, within the bound.
A program may use at most 128 MiB of HBM per device.

```python
import jax
import jax.numpy as jnp
from jax import lax

RESIDUES = 512
PAIR_WIDTH = 128
MIX_WIDTH = 128


def block_scale(rng, dims, split, low, top_value):
    def one(position, shards_of):
        steps = jax.random.uniform(jax.random.fold_in(jax.random.fold_in(rng, 6), position), (shards_of,), jnp.float32, low / len(split), top_value / len(split))
        return jnp.repeat(jnp.exp(steps), dims[position] // shards_of).reshape((-1,) + (1,) * (len(dims) - position - 1))

    gain = one(*split[0])
    for cut in split[1:]:
        gain = gain * one(*cut)
    return gain


def scatter_about(own_key, extent, spread, reach, pieces=(), kind=jnp.bfloat16):
    values = jax.random.normal(own_key, extent, jnp.float32) * spread
    if len(pieces) > 0:
        values = block_scale(own_key, extent, pieces, -0.22, 0.18) * values
    return jnp.clip(values, min=-reach, max=reach).astype(kind)


def setup_inputs(seed: int = 0, part: int = 0) -> dict:
    key_of = jax.random.split(jax.random.key(seed), 10)
    own_keys = jax.random.split(jax.random.fold_in(key_of[9], part), 10)
    pair_rows = scatter_about(own_keys[0], (RESIDUES, RESIDUES, PAIR_WIDTH), 1.0, 6.0, ((0, 4), (1, 16)))
    in_gain = jnp.clip(1.0 + 0.15 * jax.random.normal(key_of[1], (PAIR_WIDTH,), jnp.float32), 0.25, 1.75)
    left_weight = scatter_about(own_keys[2], (PAIR_WIDTH, MIX_WIDTH), PAIR_WIDTH ** -0.5, 0.5)
    right_weight = scatter_about(own_keys[3], (PAIR_WIDTH, MIX_WIDTH), PAIR_WIDTH ** -0.5, 0.5)
    left_gate = scatter_about(own_keys[4], (PAIR_WIDTH, MIX_WIDTH), PAIR_WIDTH ** -0.5, 0.5)
    right_gate = scatter_about(own_keys[5], (PAIR_WIDTH, MIX_WIDTH), PAIR_WIDTH ** -0.5, 0.5)
    mid_gain = jnp.clip(1.0 + 0.15 * jax.random.normal(key_of[6], (MIX_WIDTH,), jnp.float32), 0.25, 1.75)
    out_weight = scatter_about(own_keys[7], (MIX_WIDTH, PAIR_WIDTH), MIX_WIDTH ** -0.5, 0.5)
    out_gate = scatter_about(own_keys[8], (PAIR_WIDTH, PAIR_WIDTH), PAIR_WIDTH ** -0.5, 0.5)
    return {"pair_rows": pair_rows, "in_gain": in_gain, "left_weight": left_weight, "right_weight": right_weight, "left_gate": left_gate, "right_gate": right_gate, "mid_gain": mid_gain, "out_weight": out_weight, "out_gate": out_gate}


def scale_channels(values, channel_gain):
    centred = values - lax.optimization_barrier(jnp.mean(values, axis=-1, keepdims=True))
    return centred * lax.rsqrt(lax.optimization_barrier(jnp.mean(centred * centred, axis=-1, keepdims=True)) + 1e-05) * channel_gain

def make_factors(pair_in, in_gain, left_weight, right_weight, left_gate, right_gate):
    ready = scale_channels(pair_in.astype(jnp.float32), in_gain).astype(jnp.bfloat16)
    ready = lax.optimization_barrier(ready)
    left = jnp.einsum('ijc,cd->ijd', ready.astype(jnp.float32), left_weight.astype(jnp.float32))
    left = left * jax.nn.sigmoid(jnp.einsum('ijc,cd->ijd', ready.astype(jnp.float32), left_gate.astype(jnp.float32)))
    right = jnp.einsum('ijc,cd->ijd', ready.astype(jnp.float32), right_weight.astype(jnp.float32))
    right = right * jax.nn.sigmoid(jnp.einsum('ijc,cd->ijd', ready.astype(jnp.float32), right_gate.astype(jnp.float32)))
    return (ready, left.astype(jnp.bfloat16), right.astype(jnp.bfloat16))

def finish_pair(mixed, ready, mid_gain, out_weight, out_gate):
    scaled = scale_channels(mixed.astype(jnp.float32), mid_gain).astype(jnp.bfloat16)
    scaled = lax.optimization_barrier(scaled)
    gate = jax.nn.sigmoid(jnp.einsum('ijc,cd->ijd', ready.astype(jnp.float32), out_gate.astype(jnp.float32)))
    return (jnp.einsum('ijd,dc->ijc', scaled.astype(jnp.float32), out_weight.astype(jnp.float32)) * gate).astype(jnp.bfloat16)

def reference(pair_rows, in_gain, left_weight, right_weight, left_gate, right_gate, mid_gain, out_weight, out_gate):
    ready, left, right = make_factors(pair_rows, in_gain, left_weight, right_weight, left_gate, right_gate)
    left, right = lax.optimization_barrier((left, right))

    def one_channel(pair_of):
        return (jnp.dot(pair_of[0].T, pair_of[1], preferred_element_type=jnp.float32) * RESIDUES ** (-0.5)).astype(jnp.bfloat16)
    mixed = jnp.moveaxis(lax.map(one_channel, (jnp.moveaxis(left, -1, 0), jnp.moveaxis(right, -1, 0))), 0, -1)
    mixed = lax.optimization_barrier(mixed)
    return finish_pair(mixed, ready, mid_gain, out_weight, out_gate)
```

```python
import jax
import jax.numpy as jnp
from jax import lax
from jax.experimental import pallas as pl
from jax.experimental.pallas import tpu as pltpu
from jax.sharding import PartitionSpec as P

MESH = pl.DeviceIdType.MESH
F32 = jnp.float32
BF16 = jnp.bfloat16
NT = (((1,), (1,)), ((), ()))

NORTH, EAST = 4, 16
PEERS = NORTH * EAST
ROWS, COLS, WIDTH = 128, 32, 128
LINES = NORTH * ROWS
S = 36


def logistic(v):
    return 0.5 * jnp.tanh(0.5 * v) + 0.5


def turned(w):
    return w.astype(F32).T.astype(BF16)


def column(gain_ref):
    return jnp.broadcast_to(gain_ref[...], (WIDTH, WIDTH)).T


def kernel(
    x_ref, in_gain, lw, rw, lg, rg, mid_gain, ow, og, o_ref,
    rows, xt, gate, stage, wt, owt, ogt, gin, gmid,
    send1, recv1, send2, recv2, ssem1, rsem1, ssem2, rsem2,
):
    n, e = lax.axis_index("north"), lax.axis_index("east")
    me = n * EAST + e

    def peer(s):
        t = s + 1
        return lax.rem(n + lax.rem(t, NORTH), NORTH), lax.rem(e + t // NORTH, EAST)

    def each(count, fn, unroll=1):
        def step(s, c):
            fn(s)
            return c

        lax.fori_loop(0, count, step, 0, unroll=unroll)

    barrier = pltpu.get_barrier_semaphore()

    def greet(s):
        n2, e2 = peer(s)
        pl.semaphore_signal(
            barrier, 1, device_id={"north": n2, "east": e2}, device_id_type=MESH
        )

    each(PEERS - 1, greet)

    for kind, w in enumerate((lw, lg, rw, rg)):
        t = turned(w[...])
        wt[0, kind], wt[1, kind] = t[:PEERS], t[PEERS:]
    owt[...] = turned(ow[...])
    ogt[...] = turned(og[...])
    gin[...] = column(in_gain)
    gmid[...] = column(mid_gain)

    def widen(k):
        rows[pl.ds(k * S, COLS), :] = x_ref[k].astype(F32)

    each(ROWS, widen, 4)

    def norm(i):
        v = rows[pl.ds(i, ROWS, stride=S), :].T
        v = v - jnp.mean(v, axis=0, keepdims=True)
        v = v * lax.rsqrt(jnp.mean(v * v, axis=0, keepdims=True) + 1e-05) * gin[...]
        xt[:, pl.ds(pl.multiple_of(i * ROWS, ROWS), ROWS)] = v.astype(BF16)

    each(COLS, norm, 2)

    def columns(i):
        return pl.ds(pl.multiple_of(i * 2 * ROWS, 2 * ROWS), 2 * ROWS)

    def project(h):
        def pair(i):
            y = jnp.dot(
                wt[h].reshape(4 * PEERS, WIDTH), xt[:, columns(i)], preferred_element_type=F32
            )
            for kind in range(2):
                base = kind * 2 * PEERS
                f = y[base : base + PEERS] * logistic(y[base + PEERS : base + 2 * PEERS])
                for t in range(2):
                    stage[pl.ds(kind * PEERS * S + 2 * i + t, PEERS, stride=S), :] = f[
                        :, t * ROWS : (t + 1) * ROWS
                    ]

        each(COLS // 2, pair)

        def pack(p):
            for kind in range(2):
                send1[h, p, kind] = stage[
                    pl.ds(kind * PEERS * S + p * S, COLS), :
                ].astype(BF16)

        each(PEERS, pack, 2)

    def home1(h, n2, e2):
        return recv1.at[
            h,
            :,
            pl.ds(pl.multiple_of(e2 * COLS, COLS), COLS),
            pl.ds(pl.multiple_of(n2 * ROWS, ROWS), ROWS),
        ]

    def give1(h):
        def go(s):
            n2, e2 = peer(s)
            pltpu.make_async_remote_copy(
                send1.at[h, n2 * EAST + e2],
                home1(h, n, e),
                ssem1.at[h],
                rsem1.at[h],
                device_id={"north": n2, "east": e2},
                device_id_type=MESH,
            ).start()

        each(PEERS - 1, go)
        home1(h, n, e)[...] = send1[h, me]

    def piece2(h, n2, e2):
        return send2.at[
            h,
            pl.ds(pl.multiple_of(e2 * COLS, COLS), COLS),
            pl.ds(pl.multiple_of(n2 * ROWS, ROWS), ROWS),
        ]

    def give2(h):
        def go(s):
            n2, e2 = peer(s)
            pltpu.make_async_remote_copy(
                piece2(h, n2, e2),
                recv2.at[h * PEERS + me],
                ssem2.at[h],
                rsem2.at[h],
                device_id={"north": n2, "east": e2},
                device_id_type=MESH,
            ).start()

        each(PEERS - 1, go)
        recv2[h * PEERS + me] = piece2(h, n, e)[...]

    def all1(h, sem):
        ref = send1.at[h, pl.ds(0, PEERS - 1)]
        pltpu.make_async_copy(ref, ref, sem.at[h]).wait()

    def all2(h, sem):
        ref = recv2.at[pl.ds(0, PEERS - 1)]
        pltpu.make_async_copy(ref, ref, sem.at[h]).wait()

    project(0)
    pl.semaphore_wait(barrier, PEERS - 1)
    give1(0)
    project(1)
    give1(1)

    def open_gate(i):
        y = jnp.dot(ogt[...], xt[:, columns(i)], preferred_element_type=F32)
        gate[:, columns(i)] = logistic(y)

    each(COLS // 2, open_gate)

    for h in range(2):
        all1(h, rsem1)
        for half in range(2):
            lines = pl.ds(half * (LINES // 2), LINES // 2)
            m = lax.dot_general(
                recv1[h, 1], recv1[h, 0, lines, :], NT, preferred_element_type=F32
            )
            send2[h, :, lines] = (m * LINES**-0.5).astype(BF16)
        give2(h)

    for h in range(2):
        all2(h, rsem2)

    half = COLS // 2
    for part in range(2):
        here = pl.ds(part * half, half)

        def add(d, c):
            return c + recv2[d, here, :].astype(F32)

        zero = jnp.zeros((half, ROWS), F32)
        mean = lax.fori_loop(0, WIDTH, add, zero, unroll=8) * (1.0 / WIDTH)

        def square(d, c):
            v = recv2[d, here, :].astype(F32) - mean
            return c + v * v

        scale = lax.rsqrt(
            lax.fori_loop(0, WIDTH, square, zero, unroll=8) * (1.0 / WIDTH) + 1e-05
        )

        def spread(d):
            v = (recv2[d, here, :].astype(F32) - mean) * scale
            stage[pl.ds(d * S + part * half, half), :] = v

        each(WIDTH, spread, 8)

    def finish(j):
        s = [
            (stage[pl.ds(2 * j + t, WIDTH, stride=S), :] * gmid[...]).astype(BF16)
            for t in range(2)
        ]
        y = jnp.dot(owt[...], jnp.concatenate(s, axis=1), preferred_element_type=F32)
        y = y * gate[:, columns(j)]
        for t in range(2):
            rows[pl.ds(2 * j + t, ROWS, stride=S), :] = y[:, t * ROWS : (t + 1) * ROWS].T

    each(COLS // 2, finish)

    def narrow(i):
        o_ref[i] = rows[pl.ds(i * S, COLS), :].astype(BF16)

    each(ROWS, narrow, 4)

    for h in range(2):
        all1(h, ssem1)
        all2(h, ssem2)


def body(x, in_gain, lw, rw, lg, rg, mid_gain, ow, og):
    vmem = pl.BlockSpec(memory_space=pltpu.VMEM)
    return pl.pallas_call(
        kernel,
        out_shape=jax.ShapeDtypeStruct(x.shape, BF16),
        in_specs=[vmem] * 9,
        out_specs=vmem,
        scratch_shapes=[
            pltpu.VMEM((ROWS * S, WIDTH), F32),
            pltpu.VMEM((WIDTH, COLS * ROWS), BF16),
            pltpu.VMEM((WIDTH, COLS * ROWS), F32),
            pltpu.VMEM((WIDTH * S, ROWS), F32),
            pltpu.VMEM((2, 4, PEERS, WIDTH), BF16),
            pltpu.VMEM((WIDTH, WIDTH), BF16),
            pltpu.VMEM((WIDTH, WIDTH), BF16),
            pltpu.VMEM((WIDTH, WIDTH), F32),
            pltpu.VMEM((WIDTH, WIDTH), F32),
            pltpu.VMEM((2, PEERS, 2, COLS, ROWS), BF16),
            pltpu.VMEM((2, 2, LINES, LINES), BF16),
            pltpu.VMEM((2, LINES, LINES), BF16),
            pltpu.VMEM((WIDTH, COLS, ROWS), BF16),
            pltpu.SemaphoreType.DMA((2,)),
            pltpu.SemaphoreType.DMA((2,)),
            pltpu.SemaphoreType.DMA((2,)),
            pltpu.SemaphoreType.DMA((2,)),
        ],
        compiler_params=pltpu.CompilerParams(
            collective_id=0, has_side_effects=True, vmem_limit_bytes=40 * 2**20
        ),
        name="triangle",
    )(x, in_gain.reshape(1, WIDTH), lw, rw, lg, rg, mid_gain.reshape(1, WIDTH), ow, og)


def solution(mesh):
    placed = (P(("unit", "north"), "east", None), P()) + (P("unit", None),) * 4
    placed += (P(),) + (P("unit", None),) * 2
    return jax.shard_map(
        body,
        mesh=mesh,
        in_specs=placed,
        out_specs=P(("unit", "north"), "east", None),
        check_vma=False,
    )
```

```python
import jax
import jax.numpy as jnp
from jax import lax
from jax.experimental import pallas as pl
from jax.experimental.pallas import tpu as pltpu
from jax.sharding import PartitionSpec as P

MESH = pl.DeviceIdType.MESH
F32 = jnp.float32
BF16 = jnp.bfloat16
NT = (((1,), (1,)), ((), ()))

NORTH, EAST = 4, 16
CHIPS, CORES = 8, 2
PEERS = NORTH * EAST
GROUP = PEERS // CORES
ROWS, COLS, WIDTH = 128, 32, 128
LINES = NORTH * ROWS
S = 36


def logistic(v):
    return 0.5 * jnp.tanh(0.5 * v) + 0.5


def turned(w):
    return w.astype(F32).T.astype(BF16)


def column(gain):
    return jnp.broadcast_to(gain, (WIDTH, WIDTH)).T


def kernel(
    x_hbm, in_gain_hbm, lw_hbm, rw_hbm, lg_hbm, rg_hbm, mid_gain_hbm, ow_hbm, og_hbm, o_ref,
    x_ref, weights, gains, rows, xt, gate, stage, wt, owt, ogt, gin, gmid,
    send1, recv1, send2, recv2, lsem, near, ssem1, rsem1, ssem2, rsem2,
):
    n, e = lax.axis_index("north"), lax.axis_index("east")
    z, core = e // CORES, lax.rem(e, CORES)

    def owner(n2, e2):
        return lax.rem(e2, CORES) * GROUP + n2 * CHIPS + e2 // CORES

    me = owner(n, e)

    def each(count, fn, unroll=1, start=0):
        def step(s, c):
            fn(s)
            return c

        lax.fori_loop(start, count, step, 0, unroll=unroll)

    loads = [pltpu.make_async_copy(x_hbm, x_ref, lsem.at[0])]
    for i, w in enumerate((lw_hbm, lg_hbm, rw_hbm, rg_hbm, ow_hbm, og_hbm)):
        loads.append(pltpu.make_async_copy(w, weights.at[i], lsem.at[1 + i]))
    for i, g in enumerate((in_gain_hbm, mid_gain_hbm)):
        loads.append(pltpu.make_async_copy(g, gains.at[i], lsem.at[7 + i]))
    for load in loads:
        load.start()

    barrier = pltpu.get_barrier_semaphore()

    def greet_row(s):
        pl.semaphore_signal(
            barrier,
            1,
            device_id={"north": n, "east": lax.rem(e + s, EAST)},
            device_id_type=MESH,
        )

    def greet_column(sem):
        def go(s):
            pl.semaphore_signal(
                sem,
                1,
                device_id={"north": lax.rem(n + s, NORTH), "east": e},
                device_id_type=MESH,
            )

        each(NORTH, go, start=1)

    each(EAST, greet_row, start=1)
    greet_column(barrier)
    for load in loads:
        load.wait()

    for kind in range(4):
        t = turned(weights[kind])
        for h in range(2):
            for c in range(CORES):
                first = h * PEERS + c * GROUP
                wt[h, c, kind] = t[first : first + GROUP]
    owt[...] = turned(weights[4])
    ogt[...] = turned(weights[5])
    gin[...] = column(gains[0])
    gmid[...] = column(gains[1])

    def widen(k):
        rows[pl.ds(k * S, COLS), :] = x_ref[k].astype(F32)

    each(ROWS, widen, 4)

    def norm(i):
        v = rows[pl.ds(i, ROWS, stride=S), :].T
        v = v - jnp.mean(v, axis=0, keepdims=True)
        v = v * lax.rsqrt(jnp.mean(v * v, axis=0, keepdims=True) + 1e-05) * gin[...]
        xt[:, pl.ds(pl.multiple_of(i * ROWS, ROWS), ROWS)] = v.astype(BF16)

    each(COLS, norm, 2)

    def columns(i):
        return pl.ds(pl.multiple_of(i * 2 * ROWS, 2 * ROWS), 2 * ROWS)

    def project(h, c):
        def pair(i):
            y = jnp.dot(
                wt[h, c].reshape(4 * GROUP, WIDTH), xt[:, columns(i)], preferred_element_type=F32
            )
            for kind in range(2):
                base = kind * 2 * GROUP
                f = y[base : base + GROUP] * logistic(y[base + GROUP : base + 2 * GROUP])
                for t in range(2):
                    stage[pl.ds(kind * GROUP * S + 2 * i + t, GROUP, stride=S), :] = f[
                        :, t * ROWS : (t + 1) * ROWS
                    ]

        each(COLS // 2, pair, 2)

        def pack(p):
            for kind in range(2):
                send1[h, c * GROUP + p, kind] = stage[
                    pl.ds((kind * GROUP + p) * S, COLS), :
                ].astype(BF16)

        each(GROUP, pack, 4)

    def home1(h, n2, e2):
        return recv1.at[
            h,
            :,
            pl.ds(pl.multiple_of(e2 * COLS, COLS), COLS),
            pl.ds(pl.multiple_of(n2 * ROWS, ROWS), ROWS),
        ]

    def give1(h, c):
        def go(s):
            n2 = lax.rem(n + lax.rem(s, NORTH), NORTH)
            e2 = lax.rem(z + s // NORTH, CHIPS) * CORES + c
            pltpu.make_async_remote_copy(
                send1.at[h, owner(n2, e2)],
                home1(h, n, e),
                ssem1.at[h],
                rsem1.at[h],
                device_id={"north": n2, "east": e2},
                device_id_type=MESH,
            ).start()

        each(GROUP, go, start=1 - lax.rem(c + core, CORES))

    def piece2(h, n2, e2, first, count):
        return send2.at[
            h,
            pl.ds(pl.multiple_of(e2 * COLS + first, count), count),
            pl.ds(pl.multiple_of(n2 * ROWS, ROWS), ROWS),
        ]

    def give2(h, turn, first, count):
        def go(s):
            n2 = lax.rem(n + lax.rem(s, NORTH), NORTH)
            e2 = lax.rem(e + s // NORTH, EAST)
            pltpu.make_async_remote_copy(
                piece2(h, n2, e2, first, count),
                recv2.at[h * PEERS + me, pl.ds(first, count)],
                ssem2.at[turn],
                rsem2.at[turn],
                device_id={"north": n2, "east": e2},
                device_id_type=MESH,
            ).start()

        each(PEERS, go, start=1)

    def all1(h, sem):
        ref = send1.at[h, pl.ds(0, PEERS - 1)]
        pltpu.make_async_copy(ref, ref, sem.at[h]).wait()

    def all2(turn, sem):
        ref = recv2.at[pl.ds(0, PEERS - 1), pl.ds(0, COLS if turn == 0 else COLS // 2)]
        pltpu.make_async_copy(ref, ref, sem.at[turn]).wait()

    project(0, 0)
    pl.semaphore_wait(barrier, EAST - 1 + NORTH - 1)
    greet_column(near)
    pl.semaphore_wait(near, NORTH - 1)
    give1(0, 0)
    project(0, 1)
    give1(0, 1)
    project(1, 0)
    give1(1, 0)
    project(1, 1)
    give1(1, 1)
    for h in range(2):
        home1(h, n, e)[...] = send1[h, me]

    def open_gate(i):
        y = jnp.dot(ogt[...], xt[:, columns(i)], preferred_element_type=F32)
        gate[:, columns(i)] = logistic(y)

    each(COLS // 2, open_gate)

    for h in range(2):
        all1(h, rsem1)
        for half in range(2):
            lines = pl.ds(half * (LINES // 2), LINES // 2)
            m = lax.dot_general(
                recv1[h, 1], recv1[h, 0, lines, :], NT, preferred_element_type=F32
            )
            send2[h, :, lines] = (m * LINES**-0.5).astype(BF16)
        recv2[h * PEERS + me] = piece2(h, n, e, 0, COLS)[...]
        if h == 0:
            give2(0, 0, 0, COLS)
        else:
            give2(1, 1, 0, COLS // 2)
            give2(1, 2, COLS // 2, COLS // 2)

    half = COLS // 2
    all2(0, rsem2)
    for part in range(2):
        all2(1 + part, rsem2)
        here = pl.ds(part * half, half)

        def add(d, c):
            return c + recv2[d, here, :].astype(F32)

        zero = jnp.zeros((half, ROWS), F32)
        mean = lax.fori_loop(0, WIDTH, add, zero, unroll=8) * (1.0 / WIDTH)

        def square(d, c):
            v = recv2[d, here, :].astype(F32) - mean
            return c + v * v

        scale = lax.rsqrt(
            lax.fori_loop(0, WIDTH, square, zero, unroll=8) * (1.0 / WIDTH) + 1e-05
        )

        def spread(d):
            v = (recv2[d, here, :].astype(F32) - mean) * scale
            stage[pl.ds(d * S + part * half, half), :] = v

        each(WIDTH, spread, 8)

        def finish(jj):
            j = part * (half // 2) + jj
            s = [
                (stage[pl.ds(2 * j + t, WIDTH, stride=S), :] * gmid[...]).astype(BF16)
                for t in range(2)
            ]
            y = jnp.dot(owt[...], jnp.concatenate(s, axis=1), preferred_element_type=F32)
            y = y * gate[:, columns(j)]
            for t in range(2):
                rows[pl.ds(2 * j + t, ROWS, stride=S), :] = y[:, t * ROWS : (t + 1) * ROWS].T

        each(half // 2, finish, 2)

        def narrow(i):
            o_ref[i, here, :] = rows[pl.ds(i * S + part * half, half), :].astype(BF16)

        each(ROWS, narrow, 8)

    for h in range(2):
        all1(h, ssem1)
    for turn in range(3):
        all2(turn, ssem2)


def body(x, in_gain, lw, rw, lg, rg, mid_gain, ow, og):
    vmem = pl.BlockSpec(memory_space=pltpu.VMEM)
    hbm = pl.BlockSpec(memory_space=pltpu.HBM)
    return pl.pallas_call(
        kernel,
        out_shape=jax.ShapeDtypeStruct(x.shape, BF16),
        in_specs=[hbm] * 9,
        out_specs=vmem,
        scratch_shapes=[
            pltpu.VMEM(x.shape, BF16),
            pltpu.VMEM((6, WIDTH, WIDTH), BF16),
            pltpu.VMEM((2, 1, WIDTH), F32),
            pltpu.VMEM((ROWS * S, WIDTH), F32),
            pltpu.VMEM((WIDTH, COLS * ROWS), BF16),
            pltpu.VMEM((WIDTH, COLS * ROWS), F32),
            pltpu.VMEM((WIDTH * S, ROWS), F32),
            pltpu.VMEM((2, CORES, 4, GROUP, WIDTH), BF16),
            pltpu.VMEM((WIDTH, WIDTH), BF16),
            pltpu.VMEM((WIDTH, WIDTH), BF16),
            pltpu.VMEM((WIDTH, WIDTH), F32),
            pltpu.VMEM((WIDTH, WIDTH), F32),
            pltpu.VMEM((2, PEERS, 2, COLS, ROWS), BF16),
            pltpu.VMEM((2, 2, LINES, LINES), BF16),
            pltpu.VMEM((2, LINES, LINES), BF16),
            pltpu.VMEM((WIDTH, COLS, ROWS), BF16),
            pltpu.SemaphoreType.DMA((9,)),
            pltpu.SemaphoreType.REGULAR,
            pltpu.SemaphoreType.DMA((2,)),
            pltpu.SemaphoreType.DMA((2,)),
            pltpu.SemaphoreType.DMA((3,)),
            pltpu.SemaphoreType.DMA((3,)),
        ],
        compiler_params=pltpu.CompilerParams(
            collective_id=0, has_side_effects=True, vmem_limit_bytes=40 * 2**20
        ),
        name="triangle",
    )(x, in_gain.reshape(1, WIDTH), lw, rw, lg, rg, mid_gain.reshape(1, WIDTH), ow, og)


def solution(mesh):
    placed = (P(("unit", "north"), "east", None), P()) + (P("unit", None),) * 4
    placed += (P(),) + (P("unit", None),) * 2
    return jax.shard_map(
        body,
        mesh=mesh,
        in_specs=placed,
        out_specs=P(("unit", "north"), "east", None),
        check_vma=False,
    )
```

```python
import jax
import jax.numpy as jnp
from jax import lax
from jax.experimental import pallas as pl
from jax.experimental.pallas import tpu as pltpu
from jax.sharding import PartitionSpec as P

MESH = pl.DeviceIdType.MESH
F32 = jnp.float32
BF16 = jnp.bfloat16
NT = (((1,), (1,)), ((), ()))

NORTH, EAST = 4, 16
CHIPS, CORES = 8, 2
PEERS = NORTH * EAST
GROUP = PEERS // CORES
ROWS, COLS, WIDTH = 128, 32, 128
LINES = NORTH * ROWS
S = 36


def logistic(v):
    return 0.5 * jnp.tanh(0.5 * v) + 0.5


def turned(w):
    return w.astype(F32).T.astype(BF16)


def column(gain):
    return jnp.broadcast_to(gain, (WIDTH, WIDTH)).T


def kernel(
    x_hbm, in_gain_hbm, lw_hbm, rw_hbm, lg_hbm, rg_hbm, mid_gain_hbm, ow_hbm, og_hbm, o_ref,
    x_ref, weights, gains, rows, xt, gate, stage, wt, owt, ogt, gin, gmid,
    send1, recv1, send2, recv2, lsem, ssem1, rsem1, ssem2, rsem2,
):
    n, e = lax.axis_index("north"), lax.axis_index("east")
    z, core = e // CORES, lax.rem(e, CORES)

    def owner(n2, e2):
        return lax.rem(e2, CORES) * GROUP + n2 * CHIPS + e2 // CORES

    me = owner(n, e)

    def each(count, fn, unroll=1, start=0):
        def step(s, c):
            fn(s)
            return c

        lax.fori_loop(start, count, step, 0, unroll=unroll)

    loads = [pltpu.make_async_copy(x_hbm, x_ref, lsem.at[0])]
    for i, w in enumerate((lw_hbm, lg_hbm, rw_hbm, rg_hbm, ow_hbm, og_hbm)):
        loads.append(pltpu.make_async_copy(w, weights.at[i], lsem.at[1 + i]))
    for i, g in enumerate((in_gain_hbm, mid_gain_hbm)):
        loads.append(pltpu.make_async_copy(g, gains.at[i], lsem.at[7 + i]))
    for load in loads:
        load.start()

    barrier = pltpu.get_barrier_semaphore()

    def greet(s):
        n2 = lax.rem(n + lax.rem(s, NORTH), NORTH)
        e2 = lax.rem(e + s // NORTH, EAST)
        pl.semaphore_signal(
            barrier, 1, device_id={"north": n2, "east": e2}, device_id_type=MESH
        )

    each(PEERS, greet, start=1)
    for load in loads:
        load.wait()

    for kind in range(4):
        t = turned(weights[kind])
        for h in range(2):
            for c in range(CORES):
                first = h * PEERS + c * GROUP
                wt[h, c, kind] = t[first : first + GROUP]
    owt[...] = turned(weights[4])
    ogt[...] = turned(weights[5])
    gin[...] = column(gains[0])
    gmid[...] = column(gains[1])

    def widen(k):
        rows[pl.ds(k * S, COLS), :] = x_ref[k].astype(F32)

    each(ROWS, widen, 4)

    def norm(i):
        v = rows[pl.ds(i, ROWS, stride=S), :].T
        v = v - jnp.mean(v, axis=0, keepdims=True)
        v = v * lax.rsqrt(jnp.mean(v * v, axis=0, keepdims=True) + 1e-05) * gin[...]
        xt[:, pl.ds(pl.multiple_of(i * ROWS, ROWS), ROWS)] = v.astype(BF16)

    each(COLS, norm, 2)

    def columns(i):
        return pl.ds(pl.multiple_of(i * 2 * ROWS, 2 * ROWS), 2 * ROWS)

    def project(h, c):
        def pair(i):
            y = jnp.dot(
                wt[h, c].reshape(4 * GROUP, WIDTH), xt[:, columns(i)], preferred_element_type=F32
            )
            for kind in range(2):
                base = kind * 2 * GROUP
                f = y[base : base + GROUP] * logistic(y[base + GROUP : base + 2 * GROUP])
                for t in range(2):
                    stage[pl.ds(kind * GROUP * S + 2 * i + t, GROUP, stride=S), :] = f[
                        :, t * ROWS : (t + 1) * ROWS
                    ]

        each(COLS // 2, pair, 2)

        def pack(p):
            for kind in range(2):
                send1[h, c * GROUP + p, kind] = stage[
                    pl.ds((kind * GROUP + p) * S, COLS), :
                ].astype(BF16)

        each(GROUP, pack, 4)

    def home1(h, n2, e2):
        return recv1.at[
            h,
            :,
            pl.ds(pl.multiple_of(e2 * COLS, COLS), COLS),
            pl.ds(pl.multiple_of(n2 * ROWS, ROWS), ROWS),
        ]

    def give1(h, c):
        def go(s):
            n2 = lax.rem(n + lax.rem(s, NORTH), NORTH)
            e2 = lax.rem(z + s // NORTH, CHIPS) * CORES + c
            pltpu.make_async_remote_copy(
                send1.at[h, owner(n2, e2)],
                home1(h, n, e),
                ssem1.at[h],
                rsem1.at[h],
                device_id={"north": n2, "east": e2},
                device_id_type=MESH,
            ).start()

        each(GROUP, go, start=1 - lax.rem(c + core, CORES))

    def piece2(h, n2, e2, first, count):
        return send2.at[
            h,
            pl.ds(pl.multiple_of(e2 * COLS + first, count), count),
            pl.ds(pl.multiple_of(n2 * ROWS, ROWS), ROWS),
        ]

    def give2(h, turn, first, count):
        def go(s):
            n2 = lax.rem(n + lax.rem(s, NORTH), NORTH)
            e2 = lax.rem(e + s // NORTH, EAST)
            pltpu.make_async_remote_copy(
                piece2(h, n2, e2, first, count),
                recv2.at[h * PEERS + me, pl.ds(first, count)],
                ssem2.at[turn],
                rsem2.at[turn],
                device_id={"north": n2, "east": e2},
                device_id_type=MESH,
            ).start()

        each(PEERS, go, start=1)

    def all1(h, sem):
        ref = send1.at[h, pl.ds(0, PEERS - 1)]
        pltpu.make_async_copy(ref, ref, sem.at[h]).wait()

    def all2(turn, sem):
        ref = recv2.at[pl.ds(0, PEERS - 1), pl.ds(0, COLS if turn == 0 else COLS // 2)]
        pltpu.make_async_copy(ref, ref, sem.at[turn]).wait()

    project(0, 0)
    pl.semaphore_wait(barrier, PEERS - 1)
    give1(0, 0)
    project(0, 1)
    give1(0, 1)
    project(1, 0)
    give1(1, 0)
    project(1, 1)
    give1(1, 1)
    for h in range(2):
        home1(h, n, e)[...] = send1[h, me]

    def open_gate(i):
        y = jnp.dot(ogt[...], xt[:, columns(i)], preferred_element_type=F32)
        gate[:, columns(i)] = logistic(y)

    each(COLS // 2, open_gate)

    for h in range(2):
        all1(h, rsem1)
        for half in range(2):
            lines = pl.ds(half * (LINES // 2), LINES // 2)
            m = lax.dot_general(
                recv1[h, 1], recv1[h, 0, lines, :], NT, preferred_element_type=F32
            )
            send2[h, :, lines] = (m * LINES**-0.5).astype(BF16)
        recv2[h * PEERS + me] = piece2(h, n, e, 0, COLS)[...]
        if h == 0:
            give2(0, 0, 0, COLS)
        else:
            give2(1, 1, 0, COLS // 2)
            give2(1, 2, COLS // 2, COLS // 2)

    half = COLS // 2
    all2(0, rsem2)
    for part in range(2):
        all2(1 + part, rsem2)
        here = pl.ds(part * half, half)

        def add(d, c):
            return c + recv2[d, here, :].astype(F32)

        zero = jnp.zeros((half, ROWS), F32)
        mean = lax.fori_loop(0, WIDTH, add, zero, unroll=8) * (1.0 / WIDTH)

        def square(d, c):
            v = recv2[d, here, :].astype(F32) - mean
            return c + v * v

        scale = lax.rsqrt(
            lax.fori_loop(0, WIDTH, square, zero, unroll=8) * (1.0 / WIDTH) + 1e-05
        )

        def spread(d):
            v = (recv2[d, here, :].astype(F32) - mean) * scale
            stage[pl.ds(d * S + part * half, half), :] = v

        each(WIDTH, spread, 8)

        def finish(jj):
            j = part * (half // 2) + jj
            s = [
                (stage[pl.ds(2 * j + t, WIDTH, stride=S), :] * gmid[...]).astype(BF16)
                for t in range(2)
            ]
            y = jnp.dot(owt[...], jnp.concatenate(s, axis=1), preferred_element_type=F32)
            y = y * gate[:, columns(j)]
            for t in range(2):
                rows[pl.ds(2 * j + t, ROWS, stride=S), :] = y[:, t * ROWS : (t + 1) * ROWS].T

        each(half // 2, finish, 2)

        def narrow(i):
            o_ref[i, here, :] = rows[pl.ds(i * S + part * half, half), :].astype(BF16)

        each(ROWS, narrow, 8)

    for h in range(2):
        all1(h, ssem1)
    for turn in range(3):
        all2(turn, ssem2)


def body(x, in_gain, lw, rw, lg, rg, mid_gain, ow, og):
    vmem = pl.BlockSpec(memory_space=pltpu.VMEM)
    hbm = pl.BlockSpec(memory_space=pltpu.HBM)
    return pl.pallas_call(
        kernel,
        out_shape=jax.ShapeDtypeStruct(x.shape, BF16),
        in_specs=[hbm] * 9,
        out_specs=vmem,
        scratch_shapes=[
            pltpu.VMEM(x.shape, BF16),
            pltpu.VMEM((6, WIDTH, WIDTH), BF16),
            pltpu.VMEM((2, 1, WIDTH), F32),
            pltpu.VMEM((ROWS * S, WIDTH), F32),
            pltpu.VMEM((WIDTH, COLS * ROWS), BF16),
            pltpu.VMEM((WIDTH, COLS * ROWS), F32),
            pltpu.VMEM((WIDTH * S, ROWS), F32),
            pltpu.VMEM((2, CORES, 4, GROUP, WIDTH), BF16),
            pltpu.VMEM((WIDTH, WIDTH), BF16),
            pltpu.VMEM((WIDTH, WIDTH), BF16),
            pltpu.VMEM((WIDTH, WIDTH), F32),
            pltpu.VMEM((WIDTH, WIDTH), F32),
            pltpu.VMEM((2, PEERS, 2, COLS, ROWS), BF16),
            pltpu.VMEM((2, 2, LINES, LINES), BF16),
            pltpu.VMEM((2, LINES, LINES), BF16),
            pltpu.VMEM((WIDTH, COLS, ROWS), BF16),
            pltpu.SemaphoreType.DMA((9,)),
            pltpu.SemaphoreType.DMA((2,)),
            pltpu.SemaphoreType.DMA((2,)),
            pltpu.SemaphoreType.DMA((3,)),
            pltpu.SemaphoreType.DMA((3,)),
        ],
        compiler_params=pltpu.CompilerParams(
            collective_id=0, has_side_effects=True, vmem_limit_bytes=64_000_000
        ),
        name="triangle",
    )(x, in_gain.reshape(1, WIDTH), lw, rw, lg, rg, mid_gain.reshape(1, WIDTH), ow, og)


def solution(mesh):
    placed = (P(("unit", "north"), "east", None), P()) + (P("unit", None),) * 4
    placed += (P(),) + (P("unit", None),) * 2
    return jax.shard_map(
        body,
        mesh=mesh,
        in_specs=placed,
        out_specs=P(("unit", "north"), "east", None),
        check_vma=False,
    )
```

```python
import jax
import jax.numpy as jnp
from jax import lax
from jax.experimental import pallas as pl
from jax.experimental.pallas import tpu as pltpu
from jax.sharding import PartitionSpec as P

MESH = pl.DeviceIdType.MESH
F32 = jnp.float32
BF16 = jnp.bfloat16
NT = (((1,), (1,)), ((), ()))

NORTH, EAST = 4, 16
CHIPS, CORES = 8, 2
PEERS = NORTH * EAST
GROUP = PEERS // CORES
REACH = 4
ROWS, COLS, WIDTH = 128, 32, 128
LINES = NORTH * ROWS
BAND = CORES * COLS
S = 36


def logistic(v):
    return 0.5 * jnp.tanh(0.5 * v) + 0.5


def turned(w):
    return w.astype(F32).T.astype(BF16)


def column(gain):
    return jnp.broadcast_to(gain, (WIDTH, WIDTH)).T


def kernel(
    x_hbm, in_gain_hbm, lw_hbm, rw_hbm, lg_hbm, rg_hbm, mid_gain_hbm, ow_hbm, og_hbm, o_ref,
    x_ref, weights, gains, rows, xt, gate, stage, wt, owt, ogt, gin, gmid,
    send1, recv1, send2, recv2, lsem, ssem1, rsem1, ssemh, rsemh, ssem2, rsem2,
):
    n, e = lax.axis_index("north"), lax.axis_index("east")
    z, core = e // CORES, lax.rem(e, CORES)

    def set_of(c, n2, z2, side):
        return c * GROUP + n2 * CHIPS + lax.rem(z2 - side + CHIPS, CHIPS)

    def away(side, steps):
        return lax.rem(z + CHIPS + (2 * side - 1) * steps, CHIPS)

    def each(count, fn, unroll=1, start=0):
        def step(s, c):
            fn(s)
            return c

        lax.fori_loop(start, count, step, 0, unroll=unroll)

    loads = [pltpu.make_async_copy(x_hbm, x_ref, lsem.at[0])]
    for i, w in enumerate((lw_hbm, lg_hbm, rw_hbm, rg_hbm, ow_hbm, og_hbm)):
        loads.append(pltpu.make_async_copy(w, weights.at[i], lsem.at[1 + i]))
    for i, g in enumerate((in_gain_hbm, mid_gain_hbm)):
        loads.append(pltpu.make_async_copy(g, gains.at[i], lsem.at[7 + i]))
    for load in loads:
        load.start()

    barrier = pltpu.get_barrier_semaphore()

    peers = (2 * REACH - 1) * CORES * NORTH

    def greet(s):
        q = peers - 1 - s
        far = q // (CORES * NORTH)
        step = (far + 1) // 2 * (1 - 2 * lax.rem(far, 2))
        e2 = lax.rem(z + CHIPS + step, CHIPS) * CORES + lax.rem(core + q // NORTH, CORES)
        pl.semaphore_signal(
            barrier,
            1,
            device_id={"north": lax.rem(n + q, NORTH), "east": e2},
            device_id_type=MESH,
        )

    each(peers - 1, greet)
    for load in loads:
        load.wait()

    for kind in range(4):
        t = turned(weights[kind])
        for h in range(2):
            for c in range(CORES):
                first = h * PEERS + c * GROUP
                wt[h, c, kind] = t[first : first + GROUP]
    owt[...] = turned(weights[4])
    ogt[...] = turned(weights[5])
    gin[...] = column(gains[0])
    gmid[...] = column(gains[1])

    def widen(k):
        rows[pl.ds(k * S, COLS), :] = x_ref[k].astype(F32)

    each(ROWS, widen, 4)

    def norm(i):
        v = rows[pl.ds(i, ROWS, stride=S), :].T
        v = v - jnp.mean(v, axis=0, keepdims=True)
        v = v * lax.rsqrt(jnp.mean(v * v, axis=0, keepdims=True) + 1e-05) * gin[...]
        xt[:, pl.ds(pl.multiple_of(i * ROWS, ROWS), ROWS)] = v.astype(BF16)

    each(COLS, norm, 2)

    def columns(i):
        return pl.ds(pl.multiple_of(i * 2 * ROWS, 2 * ROWS), 2 * ROWS)

    def project(h, c):
        def pair(i):
            y = jnp.dot(
                wt[h, c].reshape(4 * GROUP, WIDTH), xt[:, columns(i)], preferred_element_type=F32
            )
            for kind in range(2):
                base = kind * 2 * GROUP
                f = y[base : base + GROUP] * logistic(y[base + GROUP : base + 2 * GROUP])
                for t in range(2):
                    stage[pl.ds(kind * GROUP * S + 2 * i + t, GROUP, stride=S), :] = f[
                        :, t * ROWS : (t + 1) * ROWS
                    ]

        each(COLS // 2, pair, 2)

        def pack(p):
            for kind in range(2):
                send1[h, c * GROUP + p, kind] = stage[
                    pl.ds((kind * GROUP + p) * S, COLS), :
                ].astype(BF16)

        each(GROUP, pack, 4)

    def place1(h, side):
        return recv1.at[
            h,
            side,
            :,
            pl.ds(pl.multiple_of(e * COLS, COLS), COLS),
            pl.ds(pl.multiple_of(n * ROWS, ROWS), ROWS),
        ]

    def give1(h, c):
        def go(s):
            q = GROUP - 1 - s
            side, n2, steps = lax.rem(q, 2), lax.rem(n + q // 2, NORTH), q // (2 * NORTH)
            z2 = away(1 - side, steps)
            pltpu.make_async_remote_copy(
                send1.at[h, set_of(c, n2, z2, side)],
                place1(h, side),
                ssem1.at[h],
                rsem1.at[h, side],
                device_id={"north": n2, "east": z2 * CORES + c},
                device_id_type=MESH,
            ).start()

        each(GROUP - 2 * (1 - lax.rem(c + core, CORES)), go)

    def band(h, side, kind, steps):
        first = pl.multiple_of(away(side, steps) * BAND, BAND)
        return recv1.at[h, side, kind, pl.ds(first, BAND)]

    def hand(h, side):
        z2 = away(1 - side, 1)
        for steps in range(REACH):
            first = pl.multiple_of(away(side, steps) * BAND, BAND)
            pltpu.make_async_remote_copy(
                recv1.at[h, side, 0, pl.ds(first, BAND)],
                recv1.at[h, 1 - side, 0, pl.ds(first, BAND)],
                ssemh.at[h, side],
                rsemh.at[h, 1 - side],
                device_id={"north": n, "east": z2 * CORES + core},
                device_id_type=MESH,
            ).start()

    def piece2(h, side, steps, c, n2, first, count):
        return send2.at[
            h,
            side,
            pl.ds(pl.multiple_of(steps * BAND + c * COLS + first, count), count),
            pl.ds(pl.multiple_of(n2 * ROWS, ROWS), ROWS),
        ]

    def give2(h, side, turn, first, count):
        def go(s):
            q = GROUP - 1 - s
            n2, c, steps = lax.rem(n + q, NORTH), lax.rem(core + q // NORTH, CORES), q // 8
            pltpu.make_async_remote_copy(
                piece2(h, side, steps, c, n2, first, count),
                recv2.at[h * PEERS + set_of(core, n, z, side), pl.ds(first, count)],
                ssem2.at[turn],
                rsem2.at[turn],
                device_id={"north": n2, "east": away(side, steps) * CORES + c},
                device_id_type=MESH,
            ).start()

        each(GROUP - 1, go)

    def wait_for(ref, sem):
        pltpu.make_async_copy(ref, ref, sem).wait()

    def sent1(h, count):
        return send1.at[h, pl.ds(0, count)]

    def handed(h):
        return recv1.at[h, 0, 0, pl.ds(0, REACH * BAND)]

    def sent2(turn):
        return recv2.at[pl.ds(0, PEERS - 2), pl.ds(0, COLS if turn == 0 else COLS // 2)]

    project(0, 0)
    pl.semaphore_wait(barrier, peers - 1)
    give1(0, 0)
    project(0, 1)
    give1(0, 1)
    project(1, 0)
    give1(1, 0)
    project(1, 1)
    give1(1, 1)
    for h in range(2):
        for side in range(2):
            place1(h, side)[...] = send1[h, set_of(core, n, z, side)]

    def open_gate(i):
        y = jnp.dot(ogt[...], xt[:, columns(i)], preferred_element_type=F32)
        gate[:, columns(i)] = logistic(y)

    each(COLS // 2, open_gate)

    for h in range(2):
        for side in range(2):
            wait_for(sent1(h, GROUP - 1), rsem1.at[h, side])
            hand(h, side)

    for h in range(2):
        for side in range(2):
            wait_for(handed(h), rsemh.at[h, side])
            right = jnp.concatenate([band(h, side, 1, k)[...] for k in range(REACH)], axis=0)
            for part in range(2):
                lines = pl.ds(part * (LINES // 2), LINES // 2)
                m = lax.dot_general(
                    right, recv1[h, side, 0, lines, :], NT, preferred_element_type=F32
                )
                send2[h, side, :, lines] = (m * LINES**-0.5).astype(BF16)
            recv2[h * PEERS + set_of(core, n, z, side)] = piece2(
                h, side, 0, core, n, 0, COLS
            )[...]
            if h == 0:
                give2(0, side, 0, 0, COLS)
        if h == 1:
            for part in range(2):
                for side in range(2):
                    give2(1, side, 1 + part, part * (COLS // 2), COLS // 2)

    half = COLS // 2
    wait_for(sent2(0), rsem2.at[0])
    for part in range(2):
        wait_for(sent2(1 + part), rsem2.at[1 + part])
        here = pl.ds(part * half, half)

        def add(d, c):
            return c + recv2[d, here, :].astype(F32)

        zero = jnp.zeros((half, ROWS), F32)
        mean = lax.fori_loop(0, WIDTH, add, zero, unroll=8) * (1.0 / WIDTH)

        def square(d, c):
            v = recv2[d, here, :].astype(F32) - mean
            return c + v * v

        scale = lax.rsqrt(
            lax.fori_loop(0, WIDTH, square, zero, unroll=8) * (1.0 / WIDTH) + 1e-05
        )

        def spread(d):
            v = (recv2[d, here, :].astype(F32) - mean) * scale
            stage[pl.ds(d * S + part * half, half), :] = v

        each(WIDTH, spread, 8)

        def finish(jj):
            j = part * (half // 2) + jj
            s = [
                (stage[pl.ds(2 * j + t, WIDTH, stride=S), :] * gmid[...]).astype(BF16)
                for t in range(2)
            ]
            y = jnp.dot(owt[...], jnp.concatenate(s, axis=1), preferred_element_type=F32)
            y = y * gate[:, columns(j)]
            for t in range(2):
                rows[pl.ds(2 * j + t, ROWS, stride=S), :] = y[:, t * ROWS : (t + 1) * ROWS].T

        each(half // 2, finish, 2)

        def narrow(i):
            o_ref[i, here, :] = rows[pl.ds(i * S + part * half, half), :].astype(BF16)

        each(ROWS, narrow, 8)

    for h in range(2):
        wait_for(sent1(h, PEERS - 2), ssem1.at[h])
        for side in range(2):
            wait_for(handed(h), ssemh.at[h, side])
    for turn in range(3):
        wait_for(sent2(turn), ssem2.at[turn])


def body(x, in_gain, lw, rw, lg, rg, mid_gain, ow, og):
    vmem = pl.BlockSpec(memory_space=pltpu.VMEM)
    hbm = pl.BlockSpec(memory_space=pltpu.HBM)
    return pl.pallas_call(
        kernel,
        out_shape=jax.ShapeDtypeStruct(x.shape, BF16),
        in_specs=[hbm] * 9,
        out_specs=vmem,
        scratch_shapes=[
            pltpu.VMEM(x.shape, BF16),
            pltpu.VMEM((6, WIDTH, WIDTH), BF16),
            pltpu.VMEM((2, 1, WIDTH), F32),
            pltpu.VMEM((ROWS * S, WIDTH), F32),
            pltpu.VMEM((WIDTH, COLS * ROWS), BF16),
            pltpu.VMEM((WIDTH, COLS * ROWS), F32),
            pltpu.VMEM((WIDTH * S, ROWS), F32),
            pltpu.VMEM((2, CORES, 4, GROUP, WIDTH), BF16),
            pltpu.VMEM((WIDTH, WIDTH), BF16),
            pltpu.VMEM((WIDTH, WIDTH), BF16),
            pltpu.VMEM((WIDTH, WIDTH), F32),
            pltpu.VMEM((WIDTH, WIDTH), F32),
            pltpu.VMEM((2, PEERS, 2, COLS, ROWS), BF16),
            pltpu.VMEM((2, 2, 2, LINES, LINES), BF16),
            pltpu.VMEM((2, 2, REACH * BAND, LINES), BF16),
            pltpu.VMEM((WIDTH, COLS, ROWS), BF16),
            pltpu.SemaphoreType.DMA((9,)),
            pltpu.SemaphoreType.DMA((2,)),
            pltpu.SemaphoreType.DMA((2, 2)),
            pltpu.SemaphoreType.DMA((2, 2)),
            pltpu.SemaphoreType.DMA((2, 2)),
            pltpu.SemaphoreType.DMA((3,)),
            pltpu.SemaphoreType.DMA((3,)),
        ],
        compiler_params=pltpu.CompilerParams(
            collective_id=0, has_side_effects=True, vmem_limit_bytes=64_000_000
        ),
        name="triangle",
    )(x, in_gain.reshape(1, WIDTH), lw, rw, lg, rg, mid_gain.reshape(1, WIDTH), ow, og)


def solution(mesh):
    placed = (P(("unit", "north"), "east", None), P()) + (P("unit", None),) * 4
    placed += (P(),) + (P("unit", None),) * 2
    return jax.shard_map(
        body,
        mesh=mesh,
        in_specs=placed,
        out_specs=P(("unit", "north"), "east", None),
        check_vma=False,
    )
```

```python
import jax
import jax.numpy as jnp
from jax import lax
from jax.experimental import pallas as pl
from jax.experimental.pallas import tpu as pltpu
from jax.sharding import PartitionSpec as P

MESH = pl.DeviceIdType.MESH
F32 = jnp.float32
BF16 = jnp.bfloat16
NT = (((1,), (1,)), ((), ()))

NORTH, EAST = 4, 16
CHIPS, CORES = 8, 2
PEERS = NORTH * EAST
GROUP = PEERS // CORES
REACH = 4
PIECES = ((0, 16), (16, 8), (24, 8))
ROWS, COLS, WIDTH = 128, 32, 128
LINES = NORTH * ROWS
BAND = CORES * COLS
S = 36


def logistic(v):
    return 0.5 * jnp.tanh(0.5 * v) + 0.5


def turned(w):
    return w.astype(F32).T.astype(BF16)


def column(gain):
    return jnp.broadcast_to(gain, (WIDTH, WIDTH)).T


def kernel(
    x_hbm, in_gain_hbm, lw_hbm, rw_hbm, lg_hbm, rg_hbm, mid_gain_hbm, ow_hbm, og_hbm, o_ref,
    x_ref, weights, gains, rows, xt, gate, stage, wt, owt, ogt, gin, gmid,
    send1, recv1, send2, recv2, lsem, near, ssem1, rsem1, ssemh, rsemh, ssem2, rsem2,
):
    n, e = lax.axis_index("north"), lax.axis_index("east")
    z, core = e // CORES, lax.rem(e, CORES)

    def set_of(c, n2, z2, side):
        return c * GROUP + n2 * CHIPS + lax.rem(z2 - side + CHIPS, CHIPS)

    def away(side, steps):
        return lax.rem(z + CHIPS + (2 * side - 1) * steps, CHIPS)

    def each(count, fn, unroll=1, start=0):
        def step(s, c):
            fn(s)
            return c

        lax.fori_loop(start, count, step, 0, unroll=unroll)

    loads = [pltpu.make_async_copy(x_hbm, x_ref, lsem.at[0])]
    for i, w in enumerate((lw_hbm, lg_hbm, rw_hbm, rg_hbm, ow_hbm, og_hbm)):
        loads.append(pltpu.make_async_copy(w, weights.at[i], lsem.at[1 + i]))
    for i, g in enumerate((in_gain_hbm, mid_gain_hbm)):
        loads.append(pltpu.make_async_copy(g, gains.at[i], lsem.at[7 + i]))
    for load in loads:
        load.start()

    barrier = pltpu.get_barrier_semaphore()
    partner = {"north": n, "east": e + 1 - 2 * core}
    peers = (2 * REACH - 1) * NORTH

    def greet(s):
        q = peers - 1 - s
        far = q // NORTH
        step = (far + 1) // 2 * (1 - 2 * lax.rem(far, 2))
        e2 = lax.rem(z + CHIPS + step, CHIPS) * CORES + core
        pl.semaphore_signal(
            barrier,
            1,
            device_id={"north": lax.rem(n + q, NORTH), "east": e2},
            device_id_type=MESH,
        )

    each(peers - 1, greet)
    pl.semaphore_signal(barrier, 1, device_id=partner, device_id_type=MESH)
    for load in loads:
        load.wait()

    for kind in range(4):
        t = turned(weights[kind])
        for h in range(2):
            for c in range(CORES):
                first = h * PEERS + c * GROUP
                wt[h, c, kind] = t[first : first + GROUP]
    owt[...] = turned(weights[4])
    ogt[...] = turned(weights[5])
    gin[...] = column(gains[0])
    gmid[...] = column(gains[1])

    def widen(k):
        rows[pl.ds(k * S, COLS), :] = x_ref[k].astype(F32)

    each(ROWS, widen, 4)

    def norm(i):
        v = rows[pl.ds(i, ROWS, stride=S), :].T
        v = v - jnp.mean(v, axis=0, keepdims=True)
        v = v * lax.rsqrt(jnp.mean(v * v, axis=0, keepdims=True) + 1e-05) * gin[...]
        xt[:, pl.ds(pl.multiple_of(i * ROWS, ROWS), ROWS)] = v.astype(BF16)

    each(COLS, norm, 2)

    def columns(i):
        return pl.ds(pl.multiple_of(i * 2 * ROWS, 2 * ROWS), 2 * ROWS)

    def project(h, c):
        def pair(i):
            y = jnp.dot(
                wt[h, c].reshape(4 * GROUP, WIDTH), xt[:, columns(i)], preferred_element_type=F32
            )
            for kind in range(2):
                base = kind * 2 * GROUP
                f = y[base : base + GROUP] * logistic(y[base + GROUP : base + 2 * GROUP])
                for t in range(2):
                    stage[pl.ds(kind * GROUP * S + 2 * i + t, GROUP, stride=S), :] = f[
                        :, t * ROWS : (t + 1) * ROWS
                    ]

        each(COLS // 2, pair, 2)

        def pack(p):
            for kind in range(2):
                send1[h, c * GROUP + p, kind] = stage[
                    pl.ds((kind * GROUP + p) * S, COLS), :
                ].astype(BF16)

        each(GROUP, pack, 4)

    def place1(h, side):
        return recv1.at[
            h,
            side,
            :,
            pl.ds(pl.multiple_of(e * COLS, COLS), COLS),
            pl.ds(pl.multiple_of(n * ROWS, ROWS), ROWS),
        ]

    def give1(h, c):
        def go(s):
            q = GROUP - 1 - s
            side, n2, steps = lax.rem(q, 2), lax.rem(n + q // 2, NORTH), q // (2 * NORTH)
            z2 = away(1 - side, steps)
            pltpu.make_async_remote_copy(
                send1.at[h, set_of(c, n2, z2, side)],
                place1(h, side),
                ssem1.at[h],
                rsem1.at[h, side],
                device_id={"north": n2, "east": z2 * CORES + c},
                device_id_type=MESH,
            ).start()

        each(GROUP - 2 * (1 - lax.rem(c + core, CORES)), go)

    def band(h, side, kind, steps):
        first = pl.multiple_of(away(side, steps) * BAND, BAND)
        return recv1.at[h, side, kind, pl.ds(first, BAND)]

    def hand(h, side):
        z2 = away(1 - side, 1)
        for steps in range(REACH):
            first = pl.multiple_of(away(side, steps) * BAND, BAND)
            pltpu.make_async_remote_copy(
                recv1.at[h, side, 0, pl.ds(first, BAND)],
                recv1.at[h, 1 - side, 0, pl.ds(first, BAND)],
                ssemh.at[h, side],
                rsemh.at[h, 1 - side],
                device_id={"north": n, "east": z2 * CORES + core},
                device_id_type=MESH,
            ).start()

    def piece2(h, side, steps, c, n2, first, count):
        return send2.at[
            h,
            side,
            pl.ds(pl.multiple_of(steps * BAND + c * COLS + first, count), count),
            pl.ds(pl.multiple_of(n2 * ROWS, ROWS), ROWS),
        ]

    def give2(h, side, turn, first, count):
        def go(s):
            q = GROUP - 1 - s
            n2, c, steps = lax.rem(n + q, NORTH), lax.rem(core + q // NORTH, CORES), q // 8
            pltpu.make_async_remote_copy(
                piece2(h, side, steps, c, n2, first, count),
                recv2.at[h * PEERS + set_of(core, n, z, side), pl.ds(first, count)],
                ssem2.at[turn],
                rsem2.at[turn],
                device_id={"north": n2, "east": away(side, steps) * CORES + c},
                device_id_type=MESH,
            ).start()

        each(GROUP - 1, go)

    def wait_for(ref, sem):
        pltpu.make_async_copy(ref, ref, sem).wait()

    def sent1(h, count):
        return send1.at[h, pl.ds(0, count)]

    def handed(h):
        return recv1.at[h, 0, 0, pl.ds(0, REACH * BAND)]

    def sent2(turn):
        count = COLS if turn == 0 else PIECES[turn - 1][1]
        return recv2.at[pl.ds(0, PEERS - 2), pl.ds(0, count)]

    project(0, core)
    pl.semaphore_wait(barrier, peers)
    pl.semaphore_signal(near, 1, device_id=partner, device_id_type=MESH)
    give1(0, core)
    project(0, 1 - core)
    pl.semaphore_wait(near, 1)
    give1(0, 1 - core)
    project(1, core)
    give1(1, core)
    project(1, 1 - core)
    give1(1, 1 - core)
    for h in range(2):
        for side in range(2):
            place1(h, side)[...] = send1[h, set_of(core, n, z, side)]

    def open_gate(i):
        y = jnp.dot(ogt[...], xt[:, columns(i)], preferred_element_type=F32)
        gate[:, columns(i)] = logistic(y)

    each(COLS // 2, open_gate)

    for h in range(2):
        for side in range(2):
            wait_for(sent1(h, GROUP - 1), rsem1.at[h, side])
            hand(h, side)

    for h in range(2):
        for side in range(2):
            wait_for(handed(h), rsemh.at[h, side])
            right = jnp.concatenate([band(h, side, 1, k)[...] for k in range(REACH)], axis=0)
            for part in range(2):
                lines = pl.ds(part * (LINES // 2), LINES // 2)
                m = lax.dot_general(
                    right, recv1[h, side, 0, lines, :], NT, preferred_element_type=F32
                )
                send2[h, side, :, lines] = (m * LINES**-0.5).astype(BF16)
            recv2[h * PEERS + set_of(core, n, z, side)] = piece2(
                h, side, 0, core, n, 0, COLS
            )[...]
            if h == 0:
                give2(0, side, 0, 0, COLS)
        if h == 1:
            for turn, (first, count) in enumerate(PIECES):
                for side in range(2):
                    give2(1, side, 1 + turn, first, count)

    wait_for(sent2(0), rsem2.at[0])
    for turn, (first, count) in enumerate(PIECES):
        wait_for(sent2(1 + turn), rsem2.at[1 + turn])
        here = pl.ds(first, count)

        def add(d, c):
            return c + recv2[d, here, :].astype(F32)

        zero = jnp.zeros((count, ROWS), F32)
        mean = lax.fori_loop(0, WIDTH, add, zero, unroll=8) * (1.0 / WIDTH)

        def square(d, c):
            v = recv2[d, here, :].astype(F32) - mean
            return c + v * v

        scale = lax.rsqrt(
            lax.fori_loop(0, WIDTH, square, zero, unroll=8) * (1.0 / WIDTH) + 1e-05
        )

        def spread(d):
            v = (recv2[d, here, :].astype(F32) - mean) * scale
            stage[pl.ds(d * S + first, count), :] = v

        each(WIDTH, spread, 8)

        def finish(jj):
            j = first // 2 + jj
            s = [
                (stage[pl.ds(2 * j + t, WIDTH, stride=S), :] * gmid[...]).astype(BF16)
                for t in range(2)
            ]
            y = jnp.dot(owt[...], jnp.concatenate(s, axis=1), preferred_element_type=F32)
            y = y * gate[:, columns(j)]
            for t in range(2):
                rows[pl.ds(2 * j + t, ROWS, stride=S), :] = y[:, t * ROWS : (t + 1) * ROWS].T

        each(count // 2, finish, 2)

        def narrow(i):
            o_ref[i, here, :] = rows[pl.ds(i * S + first, count), :].astype(BF16)

        each(ROWS, narrow, 8)

    for h in range(2):
        wait_for(sent1(h, PEERS - 2), ssem1.at[h])
        for side in range(2):
            wait_for(handed(h), ssemh.at[h, side])
    for turn in range(1 + len(PIECES)):
        wait_for(sent2(turn), ssem2.at[turn])


def body(x, in_gain, lw, rw, lg, rg, mid_gain, ow, og):
    vmem = pl.BlockSpec(memory_space=pltpu.VMEM)
    hbm = pl.BlockSpec(memory_space=pltpu.HBM)
    operands = x, in_gain.reshape(1, WIDTH), lw, rw, lg, rg, mid_gain.reshape(1, WIDTH), ow, og
    operands = [pltpu.with_memory_space_constraint(a, pltpu.HBM) for a in operands]
    return pl.pallas_call(
        kernel,
        out_shape=jax.ShapeDtypeStruct(x.shape, BF16),
        in_specs=[hbm] * 9,
        out_specs=vmem,
        scratch_shapes=[
            pltpu.VMEM(x.shape, BF16),
            pltpu.VMEM((6, WIDTH, WIDTH), BF16),
            pltpu.VMEM((2, 1, WIDTH), F32),
            pltpu.VMEM((ROWS * S, WIDTH), F32),
            pltpu.VMEM((WIDTH, COLS * ROWS), BF16),
            pltpu.VMEM((WIDTH, COLS * ROWS), F32),
            pltpu.VMEM((WIDTH * S, ROWS), F32),
            pltpu.VMEM((2, CORES, 4, GROUP, WIDTH), BF16),
            pltpu.VMEM((WIDTH, WIDTH), BF16),
            pltpu.VMEM((WIDTH, WIDTH), BF16),
            pltpu.VMEM((WIDTH, WIDTH), F32),
            pltpu.VMEM((WIDTH, WIDTH), F32),
            pltpu.VMEM((2, PEERS, 2, COLS, ROWS), BF16),
            pltpu.VMEM((2, 2, 2, LINES, LINES), BF16),
            pltpu.VMEM((2, 2, REACH * BAND, LINES), BF16),
            pltpu.VMEM((WIDTH, COLS, ROWS), BF16),
            pltpu.SemaphoreType.DMA((9,)),
            pltpu.SemaphoreType.REGULAR,
            pltpu.SemaphoreType.DMA((2,)),
            pltpu.SemaphoreType.DMA((2, 2)),
            pltpu.SemaphoreType.DMA((2, 2)),
            pltpu.SemaphoreType.DMA((2, 2)),
            pltpu.SemaphoreType.DMA((1 + len(PIECES),)),
            pltpu.SemaphoreType.DMA((1 + len(PIECES),)),
        ],
        compiler_params=pltpu.CompilerParams(
            collective_id=0, has_side_effects=True, vmem_limit_bytes=48_000_000
        ),
        name="triangle",
    )(*operands)


def solution(mesh):
    placed = (P(("unit", "north"), "east", None), P()) + (P("unit", None),) * 4
    placed += (P(),) + (P("unit", None),) * 2
    return jax.shard_map(
        body,
        mesh=mesh,
        in_specs=placed,
        out_specs=P(("unit", "north"), "east", None),
        check_vma=False,
    )
```

```python
import jax
import jax.numpy as jnp
from jax import lax
from jax.experimental import pallas as pl
from jax.experimental.pallas import tpu as pltpu
from jax.sharding import PartitionSpec as P

MESH = pl.DeviceIdType.MESH
F32 = jnp.float32
BF16 = jnp.bfloat16
NT = (((1,), (1,)), ((), ()))

NORTH, EAST = 4, 16
CHIPS, CORES = 8, 2
PEERS = NORTH * EAST
GROUP = PEERS // CORES
REACH = 4
PIECES = ((0, 16), (16, 8), (24, 8))
ROWS, COLS, WIDTH = 128, 32, 128
LINES = NORTH * ROWS
BAND = CORES * COLS
S = 36


def logistic(v):
    return 0.5 * jnp.tanh(0.5 * v) + 0.5


def turned(w):
    return w.astype(F32).T.astype(BF16)


def column(gain):
    return jnp.broadcast_to(gain, (WIDTH, WIDTH)).T


def kernel(
    x_hbm, in_gain_hbm, lw_hbm, rw_hbm, lg_hbm, rg_hbm, mid_gain_hbm, ow_hbm, og_hbm, o_ref,
    x_ref, weights, gains, rows, xt, gate, stage, wt, owt, ogt, gin, gmid,
    send1, recv1, send2, recv2, lsem, near, ssem1, rsem1, ssemh, rsemh, ssem2, rsem2,
):
    n, e = lax.axis_index("north"), lax.axis_index("east")
    z, core = e // CORES, lax.rem(e, CORES)

    def set_of(c, n2, z2, side):
        return c * GROUP + n2 * CHIPS + lax.rem(z2 - side + CHIPS, CHIPS)

    def away(side, steps):
        return lax.rem(z + CHIPS + (2 * side - 1) * steps, CHIPS)

    def each(count, fn, unroll=1, start=0):
        def step(s, c):
            fn(s)
            return c

        lax.fori_loop(start, count, step, 0, unroll=unroll)

    loads = [pltpu.make_async_copy(x_hbm, x_ref, lsem.at[0])]
    for i, w in enumerate((lw_hbm, lg_hbm, rw_hbm, rg_hbm, ow_hbm, og_hbm)):
        loads.append(pltpu.make_async_copy(w, weights.at[i], lsem.at[1 + i]))
    for i, g in enumerate((in_gain_hbm, mid_gain_hbm)):
        loads.append(pltpu.make_async_copy(g, gains.at[i], lsem.at[7 + i]))
    for load in loads:
        load.start()

    barrier = pltpu.get_barrier_semaphore()
    partner = {"north": n, "east": e + 1 - 2 * core}
    peers = (2 * REACH - 1) * NORTH

    def greet(s):
        q = peers - 1 - s
        far = q // NORTH
        step = (far + 1) // 2 * (1 - 2 * lax.rem(far, 2))
        e2 = lax.rem(z + CHIPS + step, CHIPS) * CORES + core
        pl.semaphore_signal(
            barrier,
            1,
            device_id={"north": lax.rem(n + q, NORTH), "east": e2},
            device_id_type=MESH,
        )

    each(peers - 1, greet)
    pl.semaphore_signal(barrier, 1, device_id=partner, device_id_type=MESH)
    for load in loads:
        load.wait()

    for kind in range(4):
        t = turned(weights[kind])
        for h in range(2):
            for c in range(CORES):
                first = h * PEERS + c * GROUP
                wt[h, c, kind] = t[first : first + GROUP]
    owt[...] = turned(weights[4])
    ogt[...] = turned(weights[5])
    gin[...] = column(gains[0])
    gmid[...] = column(gains[1])

    def widen(k):
        rows[pl.ds(k * S, COLS), :] = x_ref[k].astype(F32)

    each(ROWS, widen, 16)

    def norm(i):
        v = rows[pl.ds(i, ROWS, stride=S), :].T
        v = v - jnp.mean(v, axis=0, keepdims=True)
        v = v * lax.rsqrt(jnp.mean(v * v, axis=0, keepdims=True) + 1e-05) * gin[...]
        xt[:, pl.ds(pl.multiple_of(i * ROWS, ROWS), ROWS)] = v.astype(BF16)

    each(COLS, norm, 16)

    def columns(i):
        return pl.ds(pl.multiple_of(i * 2 * ROWS, 2 * ROWS), 2 * ROWS)

    def project(h, c):
        def pair(i):
            y = jnp.dot(
                wt[h, c].reshape(4 * GROUP, WIDTH), xt[:, columns(i)], preferred_element_type=F32
            )
            for kind in range(2):
                base = kind * 2 * GROUP
                f = y[base : base + GROUP] * logistic(y[base + GROUP : base + 2 * GROUP])
                for t in range(2):
                    stage[pl.ds(kind * GROUP * S + 2 * i + t, GROUP, stride=S), :] = f[
                        :, t * ROWS : (t + 1) * ROWS
                    ]

        each(COLS // 2, pair, 16)

        def pack(p):
            for kind in range(2):
                send1[h, c * GROUP + p, kind] = stage[
                    pl.ds((kind * GROUP + p) * S, COLS), :
                ].astype(BF16)

        each(GROUP, pack, 16)

    def place1(h, side):
        return recv1.at[
            h,
            side,
            :,
            pl.ds(pl.multiple_of(e * COLS, COLS), COLS),
            pl.ds(pl.multiple_of(n * ROWS, ROWS), ROWS),
        ]

    def give1(h, c):
        def go(s):
            q = GROUP - 1 - s
            side, n2, steps = lax.rem(q, 2), lax.rem(n + q // 2, NORTH), q // (2 * NORTH)
            z2 = away(1 - side, steps)
            pltpu.make_async_remote_copy(
                send1.at[h, set_of(c, n2, z2, side)],
                place1(h, side),
                ssem1.at[h],
                rsem1.at[h, side],
                device_id={"north": n2, "east": z2 * CORES + c},
                device_id_type=MESH,
            ).start()

        each(GROUP - 2 * (1 - lax.rem(c + core, CORES)), go)

    def band(h, side, kind, steps):
        first = pl.multiple_of(away(side, steps) * BAND, BAND)
        return recv1.at[h, side, kind, pl.ds(first, BAND)]

    def hand(h, side):
        z2 = away(1 - side, 1)
        for steps in range(REACH):
            first = pl.multiple_of(away(side, steps) * BAND, BAND)
            pltpu.make_async_remote_copy(
                recv1.at[h, side, 0, pl.ds(first, BAND)],
                recv1.at[h, 1 - side, 0, pl.ds(first, BAND)],
                ssemh.at[h, side],
                rsemh.at[h, 1 - side],
                device_id={"north": n, "east": z2 * CORES + core},
                device_id_type=MESH,
            ).start()

    def piece2(h, side, steps, c, n2, first, count):
        return send2.at[
            h,
            side,
            pl.ds(pl.multiple_of(steps * BAND + c * COLS + first, count), count),
            pl.ds(pl.multiple_of(n2 * ROWS, ROWS), ROWS),
        ]

    def give2(h, side, turn, first, count):
        def go(s):
            q = GROUP - 1 - s
            n2, c, steps = lax.rem(n + q, NORTH), lax.rem(core + q // NORTH, CORES), q // 8
            pltpu.make_async_remote_copy(
                piece2(h, side, steps, c, n2, first, count),
                recv2.at[h * PEERS + set_of(core, n, z, side), pl.ds(first, count)],
                ssem2.at[turn],
                rsem2.at[turn],
                device_id={"north": n2, "east": away(side, steps) * CORES + c},
                device_id_type=MESH,
            ).start()

        each(GROUP - 1, go)

    def wait_for(ref, sem):
        pltpu.make_async_copy(ref, ref, sem).wait()

    def sent1(h, count):
        return send1.at[h, pl.ds(0, count)]

    def handed(h):
        return recv1.at[h, 0, 0, pl.ds(0, REACH * BAND)]

    def sent2(turn):
        count = COLS if turn == 0 else PIECES[turn - 1][1]
        return recv2.at[pl.ds(0, PEERS - 2), pl.ds(0, count)]

    project(0, core)
    pl.semaphore_wait(barrier, peers)
    pl.semaphore_signal(near, 1, device_id=partner, device_id_type=MESH)
    give1(0, core)
    project(0, 1 - core)
    pl.semaphore_wait(near, 1)
    give1(0, 1 - core)
    project(1, core)
    give1(1, core)
    project(1, 1 - core)
    give1(1, 1 - core)
    for h in range(2):
        for side in range(2):
            place1(h, side)[...] = send1[h, set_of(core, n, z, side)]

    def open_gate(i):
        y = jnp.dot(ogt[...], xt[:, columns(i)], preferred_element_type=F32)
        gate[:, columns(i)] = logistic(y)

    each(COLS // 2, open_gate, 4)

    for h in range(2):
        for side in range(2):
            wait_for(sent1(h, GROUP - 1), rsem1.at[h, side])
            hand(h, side)

    for h in range(2):
        for side in range(2):
            wait_for(handed(h), rsemh.at[h, side])
            right = jnp.concatenate([band(h, side, 1, k)[...] for k in range(REACH)], axis=0)
            for part in range(2):
                lines = pl.ds(part * (LINES // 2), LINES // 2)
                m = lax.dot_general(
                    right, recv1[h, side, 0, lines, :], NT, preferred_element_type=F32
                )
                send2[h, side, :, lines] = (m * LINES**-0.5).astype(BF16)
            recv2[h * PEERS + set_of(core, n, z, side)] = piece2(
                h, side, 0, core, n, 0, COLS
            )[...]
            if h == 0:
                give2(0, side, 0, 0, COLS)
        if h == 1:
            for turn, (first, count) in enumerate(PIECES):
                for side in range(2):
                    give2(1, side, 1 + turn, first, count)

    wait_for(sent2(0), rsem2.at[0])
    for turn, (first, count) in enumerate(PIECES):
        wait_for(sent2(1 + turn), rsem2.at[1 + turn])
        here = pl.ds(first, count)

        def add(d, c):
            return c + recv2[d, here, :].astype(F32)

        zero = jnp.zeros((count, ROWS), F32)
        mean = lax.fori_loop(0, WIDTH, add, zero, unroll=16) * (1.0 / WIDTH)

        def square(d, c):
            v = recv2[d, here, :].astype(F32) - mean
            return c + v * v

        scale = lax.rsqrt(
            lax.fori_loop(0, WIDTH, square, zero, unroll=16) * (1.0 / WIDTH) + 1e-05
        )

        def spread(d):
            v = (recv2[d, here, :].astype(F32) - mean) * scale
            stage[pl.ds(d * S + first, count), :] = v

        each(WIDTH, spread, 16)

        def finish(jj):
            j = first // 2 + jj
            s = [
                (stage[pl.ds(2 * j + t, WIDTH, stride=S), :] * gmid[...]).astype(BF16)
                for t in range(2)
            ]
            y = jnp.dot(owt[...], jnp.concatenate(s, axis=1), preferred_element_type=F32)
            y = y * gate[:, columns(j)]
            for t in range(2):
                rows[pl.ds(2 * j + t, ROWS, stride=S), :] = y[:, t * ROWS : (t + 1) * ROWS].T

        each(count // 2, finish, 4)

        def narrow(i):
            o_ref[i, here, :] = rows[pl.ds(i * S + first, count), :].astype(BF16)

        each(ROWS, narrow, 16)

    for h in range(2):
        wait_for(sent1(h, PEERS - 2), ssem1.at[h])
        for side in range(2):
            wait_for(handed(h), ssemh.at[h, side])
    for turn in range(1 + len(PIECES)):
        wait_for(sent2(turn), ssem2.at[turn])


def body(x, in_gain, lw, rw, lg, rg, mid_gain, ow, og):
    vmem = pl.BlockSpec(memory_space=pltpu.VMEM)
    hbm = pl.BlockSpec(memory_space=pltpu.HBM)
    operands = x, in_gain.reshape(1, WIDTH), lw, rw, lg, rg, mid_gain.reshape(1, WIDTH), ow, og
    operands = [pltpu.with_memory_space_constraint(a, pltpu.HBM) for a in operands]
    return pl.pallas_call(
        kernel,
        out_shape=jax.ShapeDtypeStruct(x.shape, BF16),
        in_specs=[hbm] * 9,
        out_specs=vmem,
        scratch_shapes=[
            pltpu.VMEM(x.shape, BF16),
            pltpu.VMEM((6, WIDTH, WIDTH), BF16),
            pltpu.VMEM((2, 1, WIDTH), F32),
            pltpu.VMEM((ROWS * S, WIDTH), F32),
            pltpu.VMEM((WIDTH, COLS * ROWS), BF16),
            pltpu.VMEM((WIDTH, COLS * ROWS), F32),
            pltpu.VMEM((WIDTH * S, ROWS), F32),
            pltpu.VMEM((2, CORES, 4, GROUP, WIDTH), BF16),
            pltpu.VMEM((WIDTH, WIDTH), BF16),
            pltpu.VMEM((WIDTH, WIDTH), BF16),
            pltpu.VMEM((WIDTH, WIDTH), F32),
            pltpu.VMEM((WIDTH, WIDTH), F32),
            pltpu.VMEM((2, PEERS, 2, COLS, ROWS), BF16),
            pltpu.VMEM((2, 2, 2, LINES, LINES), BF16),
            pltpu.VMEM((2, 2, REACH * BAND, LINES), BF16),
            pltpu.VMEM((WIDTH, COLS, ROWS), BF16),
            pltpu.SemaphoreType.DMA((9,)),
            pltpu.SemaphoreType.REGULAR,
            pltpu.SemaphoreType.DMA((2,)),
            pltpu.SemaphoreType.DMA((2, 2)),
            pltpu.SemaphoreType.DMA((2, 2)),
            pltpu.SemaphoreType.DMA((2, 2)),
            pltpu.SemaphoreType.DMA((1 + len(PIECES),)),
            pltpu.SemaphoreType.DMA((1 + len(PIECES),)),
        ],
        compiler_params=pltpu.CompilerParams(
            collective_id=0, has_side_effects=True, vmem_limit_bytes=48_000_000
        ),
        name="triangle",
    )(*operands)


def solution(mesh):
    placed = (P(("unit", "north"), "east", None), P()) + (P("unit", None),) * 4
    placed += (P(),) + (P("unit", None),) * 2
    return jax.shard_map(
        body,
        mesh=mesh,
        in_specs=placed,
        out_specs=P(("unit", "north"), "east", None),
        check_vma=False,
    )
```

```python
import jax
import jax.numpy as jnp
from jax import lax
from jax.experimental import pallas as pl
from jax.experimental.pallas import tpu as pltpu
from jax.sharding import PartitionSpec as P

MESH = pl.DeviceIdType.MESH
F32 = jnp.float32
BF16 = jnp.bfloat16
NT = (((1,), (1,)), ((), ()))

NORTH, EAST = 4, 16
CHIPS, CORES = 8, 2
PEERS = NORTH * EAST
GROUP = PEERS // CORES
REACH = 4
PIECES = ((0, 16), (16, 8), (24, 8))
ROWS, COLS, WIDTH = 128, 32, 128
LINES = NORTH * ROWS
BAND = CORES * COLS
S = 36


def logistic(v):
    return 0.5 * jnp.tanh(0.5 * v) + 0.5


def turned(w):
    return w.astype(F32).T.astype(BF16)


def column(gain):
    return jnp.broadcast_to(gain, (WIDTH, WIDTH)).T


def kernel(
    x_hbm, in_gain_hbm, lw_hbm, rw_hbm, lg_hbm, rg_hbm, mid_gain_hbm, ow_hbm, og_hbm, o_ref,
    x_ref, weights, gains, rows, xt, gate, stage, wt, owt, ogt, gin, gmid,
    send1, recv1, send2, recv2, lsem, near_row, near, ssem1, rsem1, ssemh, rsemh, ssem2, rsem2,
):
    n, e = lax.axis_index("north"), lax.axis_index("east")
    z, core = e // CORES, lax.rem(e, CORES)

    def set_of(c, n2, z2, side):
        return c * GROUP + n2 * CHIPS + lax.rem(z2 - side + CHIPS, CHIPS)

    def away(side, steps):
        return lax.rem(z + CHIPS + (2 * side - 1) * steps, CHIPS)

    def each(count, fn, unroll=1, start=0):
        def step(s, c):
            fn(s)
            return c

        lax.fori_loop(start, count, step, 0, unroll=unroll)

    loads = [pltpu.make_async_copy(x_hbm, x_ref, lsem.at[0])]
    for i, w in enumerate((lw_hbm, lg_hbm, rw_hbm, rg_hbm, ow_hbm, og_hbm)):
        loads.append(pltpu.make_async_copy(w, weights.at[i], lsem.at[1 + i]))
    for i, g in enumerate((in_gain_hbm, mid_gain_hbm)):
        loads.append(pltpu.make_async_copy(g, gains.at[i], lsem.at[7 + i]))
    loads[0].start()

    barrier = pltpu.get_barrier_semaphore()
    partner = {"north": n, "east": e + 1 - 2 * core}
    in_row = 2 * (REACH - 1)

    def greet_row(s):
        step = (REACH - 1 - s // 2) * (1 - 2 * lax.rem(s, 2))
        e2 = lax.rem(z + CHIPS + step, CHIPS) * CORES + core
        pl.semaphore_signal(
            barrier, 1, device_id={"north": n, "east": e2}, device_id_type=MESH
        )

    def greet_column(sem):
        def go(s):
            pl.semaphore_signal(
                sem,
                1,
                device_id={"north": lax.rem(n + s, NORTH), "east": e},
                device_id_type=MESH,
            )

        each(NORTH, go, start=1)

    each(in_row, greet_row)
    greet_column(barrier)
    pl.semaphore_signal(barrier, 1, device_id=partner, device_id_type=MESH)
    for load in loads[1:]:
        load.start()
    for load in loads[1:]:
        load.wait()

    for kind in range(4):
        t = turned(weights[kind])
        for h in range(2):
            for c in range(CORES):
                first = h * PEERS + c * GROUP
                wt[h, c, kind] = t[first : first + GROUP]
    owt[...] = turned(weights[4])
    ogt[...] = turned(weights[5])
    gin[...] = column(gains[0])
    gmid[...] = column(gains[1])

    loads[0].wait()

    def widen(k):
        rows[pl.ds(k * S, COLS), :] = x_ref[k].astype(F32)

    each(ROWS, widen, 16)

    def norm(i):
        v = rows[pl.ds(i, ROWS, stride=S), :].T
        v = v - jnp.mean(v, axis=0, keepdims=True)
        v = v * lax.rsqrt(jnp.mean(v * v, axis=0, keepdims=True) + 1e-05) * gin[...]
        xt[:, pl.ds(pl.multiple_of(i * ROWS, ROWS), ROWS)] = v.astype(BF16)


    def columns(i):
        return pl.ds(pl.multiple_of(i * 2 * ROWS, 2 * ROWS), 2 * ROWS)

    def project(h, c, lo=0, hi=COLS):
        def pair(i):
            y = jnp.dot(
                wt[h, c].reshape(4 * GROUP, WIDTH), xt[:, columns(i)], preferred_element_type=F32
            )
            for kind in range(2):
                base = kind * 2 * GROUP
                f = y[base : base + GROUP] * logistic(y[base + GROUP : base + 2 * GROUP])
                for t in range(2):
                    stage[pl.ds(kind * GROUP * S + 2 * i + t, GROUP, stride=S), :] = f[
                        :, t * ROWS : (t + 1) * ROWS
                    ]

        each(hi // 2, pair, (hi - lo) // 2, start=lo // 2)

        def pack(p):
            for kind in range(2):
                send1[h, c * GROUP + p, kind, lo:hi] = stage[
                    pl.ds((kind * GROUP + p) * S + lo, hi - lo), :
                ].astype(BF16)

        each(GROUP, pack, 16)

    def place1(h, side, lo=0, hi=COLS):
        return recv1.at[
            h,
            side,
            :,
            pl.ds(pl.multiple_of(e * COLS + lo, hi - lo), hi - lo),
            pl.ds(pl.multiple_of(n * ROWS, ROWS), ROWS),
        ]

    def give1(h, c, first=0, count=NORTH, lo=0, hi=COLS):
        def go(s):
            side, steps = lax.rem(s, 2), REACH - 1 - s // (2 * count)
            n2 = lax.rem(n + first + count - 1 - lax.rem(s // 2, count), NORTH)
            z2 = away(1 - side, steps)
            pltpu.make_async_remote_copy(
                send1.at[h, set_of(c, n2, z2, side), :, pl.ds(lo, hi - lo)],
                place1(h, side, lo, hi),
                ssem1.at[h],
                rsem1.at[h, side],
                device_id={"north": n2, "east": z2 * CORES + c},
                device_id_type=MESH,
            ).start()

        own = 0 if first else 2 * (1 - lax.rem(c + core, CORES))
        each(REACH * 2 * count - own, go)

    def band(h, side, kind, steps):
        first = pl.multiple_of(away(side, steps) * BAND, BAND)
        return recv1.at[h, side, kind, pl.ds(first, BAND)]

    def hand(h, side):
        z2 = away(1 - side, 1)
        for steps in range(REACH):
            first = pl.multiple_of(away(side, steps) * BAND, BAND)
            pltpu.make_async_remote_copy(
                recv1.at[h, side, 0, pl.ds(first, BAND)],
                recv1.at[h, 1 - side, 0, pl.ds(first, BAND)],
                ssemh.at[h, side],
                rsemh.at[h, 1 - side],
                device_id={"north": n, "east": z2 * CORES + core},
                device_id_type=MESH,
            ).start()

    def piece2(h, side, steps, c, n2, first, count):
        return send2.at[
            h,
            side,
            pl.ds(pl.multiple_of(steps * BAND + c * COLS + first, count), count),
            pl.ds(pl.multiple_of(n2 * ROWS, ROWS), ROWS),
        ]

    def give2(h, side, turn, first, count):
        def go(s):
            q = GROUP - 1 - s
            n2, c, steps = lax.rem(n + q, NORTH), lax.rem(core + q // NORTH, CORES), q // 8
            pltpu.make_async_remote_copy(
                piece2(h, side, steps, c, n2, first, count),
                recv2.at[h * PEERS + set_of(core, n, z, side), pl.ds(first, count)],
                ssem2.at[turn],
                rsem2.at[turn],
                device_id={"north": n2, "east": away(side, steps) * CORES + c},
                device_id_type=MESH,
            ).start()

        each(GROUP - 1, go)

    def wait_for(ref, sem):
        pltpu.make_async_copy(ref, ref, sem).wait()

    def sent1(h, count):
        return send1.at[h, pl.ds(0, count)]

    def handed(h):
        return recv1.at[h, 0, 0, pl.ds(0, REACH * BAND)]

    def sent2(turn):
        count = COLS if turn == 0 else PIECES[turn - 1][1]
        return recv2.at[pl.ds(0, PEERS - 2), pl.ds(0, count)]

    half = COLS // 2
    each(half, norm, half)
    project(0, core, 0, half)
    pl.semaphore_wait(barrier, in_row + NORTH)
    greet_column(near_row)
    give1(0, core, 0, 1, 0, half)
    each(COLS, norm, half, start=half)
    project(0, core, half, COLS)
    pl.semaphore_wait(near_row, NORTH - 1)
    pl.semaphore_signal(near, 1, device_id=partner, device_id_type=MESH)
    give1(0, core, 1, NORTH - 1, 0, half)
    give1(0, core, 0, NORTH, half, COLS)
    project(0, 1 - core)
    pl.semaphore_wait(near, 1)
    give1(0, 1 - core)
    project(1, core)
    give1(1, core)
    project(1, 1 - core)
    give1(1, 1 - core)
    for h in range(2):
        for side in range(2):
            place1(h, side)[...] = send1[h, set_of(core, n, z, side)]

    def open_gate(i):
        y = jnp.dot(ogt[...], xt[:, columns(i)], preferred_element_type=F32)
        gate[:, columns(i)] = logistic(y)

    each(COLS // 2, open_gate, 4)

    for h in range(2):
        for side in range(2):
            wait_for(sent1(h, GROUP - 1), rsem1.at[h, side])
            hand(h, side)

    for h in range(2):
        for side in range(2):
            wait_for(handed(h), rsemh.at[h, side])
            right = jnp.concatenate([band(h, side, 1, k)[...] for k in range(REACH)], axis=0)
            for part in range(2):
                lines = pl.ds(part * (LINES // 2), LINES // 2)
                m = lax.dot_general(
                    right, recv1[h, side, 0, lines, :], NT, preferred_element_type=F32
                )
                send2[h, side, :, lines] = (m * LINES**-0.5).astype(BF16)
            recv2[h * PEERS + set_of(core, n, z, side)] = piece2(
                h, side, 0, core, n, 0, COLS
            )[...]
            if h == 0:
                give2(0, side, 0, 0, COLS)
        if h == 1:
            for turn, (first, count) in enumerate(PIECES):
                for side in range(2):
                    give2(1, side, 1 + turn, first, count)

    wait_for(sent2(0), rsem2.at[0])
    for turn, (first, count) in enumerate(PIECES):
        wait_for(sent2(1 + turn), rsem2.at[1 + turn])
        here = pl.ds(first, count)

        def tree(v):
            while v.shape[0] > 1:
                v = v[: v.shape[0] // 2] + v[v.shape[0] // 2 :]
            return v[0]

        def add(d, c):
            return c + tree(recv2[pl.ds(d * 16, 16), here, :].astype(F32))

        zero = jnp.zeros((count, ROWS), F32)
        mean = lax.fori_loop(0, WIDTH // 16, add, zero, unroll=2) * (1.0 / WIDTH)

        def square(d, c):
            v = recv2[pl.ds(d * 16, 16), here, :].astype(F32) - mean
            return c + tree(v * v)

        scale = lax.rsqrt(
            lax.fori_loop(0, WIDTH // 16, square, zero, unroll=2) * (1.0 / WIDTH) + 1e-05
        )

        def spread(d):
            v = (recv2[d, here, :].astype(F32) - mean) * scale
            stage[pl.ds(d * S + first, count), :] = v

        each(WIDTH, spread, 16)

        def finish(jj):
            j = first // 2 + jj
            s = [
                (stage[pl.ds(2 * j + t, WIDTH, stride=S), :] * gmid[...]).astype(BF16)
                for t in range(2)
            ]
            y = jnp.dot(owt[...], jnp.concatenate(s, axis=1), preferred_element_type=F32)
            y = y * gate[:, columns(j)]
            for t in range(2):
                rows[pl.ds(2 * j + t, ROWS, stride=S), :] = y[:, t * ROWS : (t + 1) * ROWS].T

        each(count // 2, finish, 4)

        def narrow(i):
            o_ref[i, here, :] = rows[pl.ds(i * S + first, count), :].astype(BF16)

        each(ROWS, narrow, 16)

    for h in range(2):
        wait_for(sent1(h, PEERS - 2), ssem1.at[h])
        for side in range(2):
            wait_for(handed(h), ssemh.at[h, side])
    for turn in range(1 + len(PIECES)):
        wait_for(sent2(turn), ssem2.at[turn])


def body(x, in_gain, lw, rw, lg, rg, mid_gain, ow, og):
    vmem = pl.BlockSpec(memory_space=pltpu.VMEM)
    hbm = pl.BlockSpec(memory_space=pltpu.HBM)
    operands = x, in_gain.reshape(1, WIDTH), lw, rw, lg, rg, mid_gain.reshape(1, WIDTH), ow, og
    operands = [pltpu.with_memory_space_constraint(a, pltpu.HBM) for a in operands]
    return pl.pallas_call(
        kernel,
        out_shape=jax.ShapeDtypeStruct(x.shape, BF16),
        in_specs=[hbm] * 9,
        out_specs=vmem,
        scratch_shapes=[
            pltpu.VMEM(x.shape, BF16),
            pltpu.VMEM((6, WIDTH, WIDTH), BF16),
            pltpu.VMEM((2, 1, WIDTH), F32),
            pltpu.VMEM((ROWS * S, WIDTH), F32),
            pltpu.VMEM((WIDTH, COLS * ROWS), BF16),
            pltpu.VMEM((WIDTH, COLS * ROWS), F32),
            pltpu.VMEM((WIDTH * S, ROWS), F32),
            pltpu.VMEM((2, CORES, 4, GROUP, WIDTH), BF16),
            pltpu.VMEM((WIDTH, WIDTH), BF16),
            pltpu.VMEM((WIDTH, WIDTH), BF16),
            pltpu.VMEM((WIDTH, WIDTH), F32),
            pltpu.VMEM((WIDTH, WIDTH), F32),
            pltpu.VMEM((2, PEERS, 2, COLS, ROWS), BF16),
            pltpu.VMEM((2, 2, 2, LINES, LINES), BF16),
            pltpu.VMEM((2, 2, REACH * BAND, LINES), BF16),
            pltpu.VMEM((WIDTH, COLS, ROWS), BF16),
            pltpu.SemaphoreType.DMA((9,)),
            pltpu.SemaphoreType.REGULAR,
            pltpu.SemaphoreType.REGULAR,
            pltpu.SemaphoreType.DMA((2,)),
            pltpu.SemaphoreType.DMA((2, 2)),
            pltpu.SemaphoreType.DMA((2, 2)),
            pltpu.SemaphoreType.DMA((2, 2)),
            pltpu.SemaphoreType.DMA((1 + len(PIECES),)),
            pltpu.SemaphoreType.DMA((1 + len(PIECES),)),
        ],
        compiler_params=pltpu.CompilerParams(
            collective_id=0, has_side_effects=True, vmem_limit_bytes=48_000_000
        ),
        name="triangle",
    )(*operands)


def solution(mesh):
    placed = (P(("unit", "north"), "east", None), P()) + (P("unit", None),) * 4
    placed += (P(),) + (P("unit", None),) * 2
    return jax.shard_map(
        body,
        mesh=mesh,
        in_specs=placed,
        out_specs=P(("unit", "north"), "east", None),
        check_vma=False,
    )
```

```python
import jax
import jax.numpy as jnp
from jax import lax
from jax.experimental import pallas as pl
from jax.experimental.pallas import tpu as pltpu
from jax.sharding import PartitionSpec as P

MESH = pl.DeviceIdType.MESH
F32 = jnp.float32
BF16 = jnp.bfloat16
NT = (((1,), (1,)), ((), ()))

NORTH, EAST = 4, 16
CHIPS, CORES = 8, 2
PEERS = NORTH * EAST
GROUP = PEERS // CORES
REACH = 4
PIECES = ((0, 8), (8, 8), (16, 8), (24, 8))
ROWS, COLS, WIDTH = 128, 32, 128
LINES = NORTH * ROWS
BAND = CORES * COLS
S = 36


def logistic(v):
    return 0.5 * jnp.tanh(0.5 * v) + 0.5


def turned(w):
    return w.astype(F32).T.astype(BF16)


def column(gain):
    return jnp.broadcast_to(gain, (WIDTH, WIDTH)).T


def kernel(
    x_hbm, in_gain_hbm, lw_hbm, rw_hbm, lg_hbm, rg_hbm, mid_gain_hbm, ow_hbm, og_hbm, o_ref,
    x_ref, weights, gains, rows, xt, gate, stage, wt, owt, ogt, gin, gmid,
    send1, recv1, send2, recv2, lsem, near_row, near, ssem1, rsem1, ssemh, rsemh, ssem2, rsem2,
):
    n, e = lax.axis_index("north"), lax.axis_index("east")
    z, core = e // CORES, lax.rem(e, CORES)

    def set_of(c, n2, z2, side):
        return c * GROUP + n2 * CHIPS + lax.rem(z2 - side + CHIPS, CHIPS)

    def away(side, steps):
        return lax.rem(z + CHIPS + (2 * side - 1) * steps, CHIPS)

    def each(count, fn, unroll=1, start=0):
        def step(s, c):
            fn(s)
            return c

        lax.fori_loop(start, count, step, 0, unroll=unroll)

    loads = [pltpu.make_async_copy(x_hbm, x_ref, lsem.at[0])]
    for i, w in enumerate((lw_hbm, lg_hbm, rw_hbm, rg_hbm, ow_hbm, og_hbm)):
        loads.append(pltpu.make_async_copy(w, weights.at[i], lsem.at[1 + i]))
    for i, g in enumerate((in_gain_hbm, mid_gain_hbm)):
        loads.append(pltpu.make_async_copy(g, gains.at[i], lsem.at[7 + i]))
    loads[0].start()

    barrier = pltpu.get_barrier_semaphore()
    partner = {"north": n, "east": e + 1 - 2 * core}
    in_row = 2 * (REACH - 1)

    def greet_row(s):
        step = (REACH - 1 - s // 2) * (1 - 2 * lax.rem(s, 2))
        e2 = lax.rem(z + CHIPS + step, CHIPS) * CORES + core
        pl.semaphore_signal(
            barrier, 1, device_id={"north": n, "east": e2}, device_id_type=MESH
        )

    def greet_column(sem):
        def go(s):
            pl.semaphore_signal(
                sem,
                1,
                device_id={"north": lax.rem(n + s, NORTH), "east": e},
                device_id_type=MESH,
            )

        each(NORTH, go, start=1)

    each(in_row, greet_row)
    greet_column(barrier)
    pl.semaphore_signal(barrier, 1, device_id=partner, device_id_type=MESH)
    for load in loads[1:]:
        load.start()
    for load in loads[1:]:
        load.wait()

    for kind in range(4):
        t = turned(weights[kind])
        for h in range(2):
            for c in range(CORES):
                first = h * PEERS + c * GROUP
                wt[h, c, kind] = t[first : first + GROUP]
    owt[...] = turned(weights[4])
    ogt[...] = turned(weights[5])
    gin[...] = column(gains[0])
    gmid[...] = column(gains[1])

    loads[0].wait()

    def widen(k):
        rows[pl.ds(k * S, COLS), :] = x_ref[k].astype(F32)

    each(ROWS, widen, 16)

    def norm(i):
        v = rows[pl.ds(i, ROWS, stride=S), :].T
        v = v - jnp.mean(v, axis=0, keepdims=True)
        v = v * lax.rsqrt(jnp.mean(v * v, axis=0, keepdims=True) + 1e-05) * gin[...]
        xt[:, pl.ds(pl.multiple_of(i * ROWS, ROWS), ROWS)] = v.astype(BF16)


    def columns(i):
        return pl.ds(pl.multiple_of(i * 2 * ROWS, 2 * ROWS), 2 * ROWS)

    def project(h, c, lo=0, hi=COLS):
        def pair(i):
            y = jnp.dot(
                wt[h, c].reshape(4 * GROUP, WIDTH), xt[:, columns(i)], preferred_element_type=F32
            )
            for kind in range(2):
                base = kind * 2 * GROUP
                f = y[base : base + GROUP] * logistic(y[base + GROUP : base + 2 * GROUP])
                for t in range(2):
                    stage[pl.ds(kind * GROUP * S + 2 * i + t, GROUP, stride=S), :] = f[
                        :, t * ROWS : (t + 1) * ROWS
                    ]

        each(hi // 2, pair, (hi - lo) // 2, start=lo // 2)

        def pack(p):
            for kind in range(2):
                send1[h, c * GROUP + p, kind, lo:hi] = stage[
                    pl.ds((kind * GROUP + p) * S + lo, hi - lo), :
                ].astype(BF16)

        each(GROUP, pack, 16)

    def place1(h, side, lo=0, hi=COLS):
        return recv1.at[
            h,
            side,
            :,
            pl.ds(pl.multiple_of(e * COLS + lo, hi - lo), hi - lo),
            pl.ds(pl.multiple_of(n * ROWS, ROWS), ROWS),
        ]

    def give1(h, c, first=0, count=NORTH, lo=0, hi=COLS):
        def go(s):
            side, steps = lax.rem(s, 2), REACH - 1 - s // (2 * count)
            n2 = lax.rem(n + first + count - 1 - lax.rem(s // 2, count), NORTH)
            z2 = away(1 - side, steps)
            pltpu.make_async_remote_copy(
                send1.at[h, set_of(c, n2, z2, side), :, pl.ds(lo, hi - lo)],
                place1(h, side, lo, hi),
                ssem1.at[h],
                rsem1.at[h, side],
                device_id={"north": n2, "east": z2 * CORES + c},
                device_id_type=MESH,
            ).start()

        own = 0 if first else 2 * (1 - lax.rem(c + core, CORES))
        each(REACH * 2 * count - own, go)

    def band(h, side, kind, steps):
        first = pl.multiple_of(away(side, steps) * BAND, BAND)
        return recv1.at[h, side, kind, pl.ds(first, BAND)]

    def hand(h, side):
        z2 = away(1 - side, 1)
        for steps in range(REACH):
            first = pl.multiple_of(away(side, steps) * BAND, BAND)
            pltpu.make_async_remote_copy(
                recv1.at[h, side, 0, pl.ds(first, BAND)],
                recv1.at[h, 1 - side, 0, pl.ds(first, BAND)],
                ssemh.at[h, side],
                rsemh.at[h, 1 - side],
                device_id={"north": n, "east": z2 * CORES + core},
                device_id_type=MESH,
            ).start()

    def piece2(h, side, steps, c, n2, first, count):
        return send2.at[
            h,
            side,
            pl.ds(pl.multiple_of(steps * BAND + c * COLS + first, count), count),
            pl.ds(pl.multiple_of(n2 * ROWS, ROWS), ROWS),
        ]

    def give2(h, side, turn, first, count):
        def go(s):
            q = GROUP - 1 - s
            n2, c, steps = lax.rem(n + q, NORTH), lax.rem(core + q // NORTH, CORES), q // 8
            pltpu.make_async_remote_copy(
                piece2(h, side, steps, c, n2, first, count),
                recv2.at[h * PEERS + set_of(core, n, z, side), pl.ds(first, count)],
                ssem2.at[turn],
                rsem2.at[turn],
                device_id={"north": n2, "east": away(side, steps) * CORES + c},
                device_id_type=MESH,
            ).start()

        each(GROUP - 1, go)

    def wait_for(ref, sem):
        pltpu.make_async_copy(ref, ref, sem).wait()

    def sent1(h, count):
        return send1.at[h, pl.ds(0, count)]

    def handed(h):
        return recv1.at[h, 0, 0, pl.ds(0, REACH * BAND)]

    def sent2(turn):
        count = COLS if turn == 0 else PIECES[turn - 1][1]
        return recv2.at[pl.ds(0, PEERS - 2), pl.ds(0, count)]

    half = COLS // 2
    each(half, norm, half)
    project(0, core, 0, half)
    pl.semaphore_wait(barrier, in_row + NORTH)
    greet_column(near_row)
    give1(0, core, 0, 1, 0, half)
    each(COLS, norm, half, start=half)
    project(0, core, half, COLS)
    pl.semaphore_wait(near_row, NORTH - 1)
    pl.semaphore_signal(near, 1, device_id=partner, device_id_type=MESH)
    give1(0, core, 1, NORTH - 1, 0, half)
    give1(0, core, 0, NORTH, half, COLS)
    project(0, 1 - core)
    pl.semaphore_wait(near, 1)
    give1(0, 1 - core)
    project(1, core)
    give1(1, core)
    project(1, 1 - core)
    give1(1, 1 - core)
    for h in range(2):
        for side in range(2):
            place1(h, side)[...] = send1[h, set_of(core, n, z, side)]

    def open_gate(i):
        y = jnp.dot(ogt[...], xt[:, columns(i)], preferred_element_type=F32)
        gate[:, columns(i)] = logistic(y)

    each(COLS // 2, open_gate, 4)

    for h in range(2):
        for side in range(2):
            wait_for(sent1(h, GROUP - 1), rsem1.at[h, side])
            hand(h, side)

    for h in range(2):
        for side in range(2):
            wait_for(handed(h), rsemh.at[h, side])
            right = jnp.concatenate([band(h, side, 1, k)[...] for k in range(REACH)], axis=0)
            for part in range(2):
                lines = pl.ds(part * (LINES // 2), LINES // 2)
                m = lax.dot_general(
                    right, recv1[h, side, 0, lines, :], NT, preferred_element_type=F32
                )
                send2[h, side, :, lines] = (m * LINES**-0.5).astype(BF16)
            recv2[h * PEERS + set_of(core, n, z, side)] = piece2(
                h, side, 0, core, n, 0, COLS
            )[...]
            if h == 0:
                give2(0, side, 0, 0, COLS)
        if h == 1:
            for turn, (first, count) in enumerate(PIECES):
                for side in range(2):
                    give2(1, side, 1 + turn, first, count)

    wait_for(sent2(0), rsem2.at[0])
    for turn, (first, count) in enumerate(PIECES):
        wait_for(sent2(1 + turn), rsem2.at[1 + turn])
        here = pl.ds(first, count)

        def tree(v):
            while v.shape[0] > 1:
                v = v[: v.shape[0] // 2] + v[v.shape[0] // 2 :]
            return v[0]

        def add(d, c):
            return c + tree(recv2[pl.ds(d * 16, 16), here, :].astype(F32))

        zero = jnp.zeros((count, ROWS), F32)
        mean = lax.fori_loop(0, WIDTH // 16, add, zero, unroll=2) * (1.0 / WIDTH)

        def square(d, c):
            v = recv2[pl.ds(d * 16, 16), here, :].astype(F32) - mean
            return c + tree(v * v)

        scale = lax.rsqrt(
            lax.fori_loop(0, WIDTH // 16, square, zero, unroll=2) * (1.0 / WIDTH) + 1e-05
        )

        def spread(d):
            v = (recv2[d, here, :].astype(F32) - mean) * scale
            stage[pl.ds(d * S + first, count), :] = v

        each(WIDTH, spread, 16)

        def finish(jj):
            j = first // 2 + jj
            s = [
                (stage[pl.ds(2 * j + t, WIDTH, stride=S), :] * gmid[...]).astype(BF16)
                for t in range(2)
            ]
            y = jnp.dot(owt[...], jnp.concatenate(s, axis=1), preferred_element_type=F32)
            y = y * gate[:, columns(j)]
            for t in range(2):
                rows[pl.ds(2 * j + t, ROWS, stride=S), :] = y[:, t * ROWS : (t + 1) * ROWS].T

        each(count // 2, finish, 4)

        def narrow(i):
            o_ref[i, here, :] = rows[pl.ds(i * S + first, count), :].astype(BF16)

        each(ROWS, narrow, 16)

    for h in range(2):
        wait_for(sent1(h, PEERS - 2), ssem1.at[h])
        for side in range(2):
            wait_for(handed(h), ssemh.at[h, side])
    for turn in range(1 + len(PIECES)):
        wait_for(sent2(turn), ssem2.at[turn])


def body(x, in_gain, lw, rw, lg, rg, mid_gain, ow, og):
    vmem = pl.BlockSpec(memory_space=pltpu.VMEM)
    hbm = pl.BlockSpec(memory_space=pltpu.HBM)
    operands = x, in_gain.reshape(1, WIDTH), lw, rw, lg, rg, mid_gain.reshape(1, WIDTH), ow, og
    operands = [pltpu.with_memory_space_constraint(a, pltpu.HBM) for a in operands]
    return pl.pallas_call(
        kernel,
        out_shape=jax.ShapeDtypeStruct(x.shape, BF16),
        in_specs=[hbm] * 9,
        out_specs=vmem,
        scratch_shapes=[
            pltpu.VMEM(x.shape, BF16),
            pltpu.VMEM((6, WIDTH, WIDTH), BF16),
            pltpu.VMEM((2, 1, WIDTH), F32),
            pltpu.VMEM((ROWS * S, WIDTH), F32),
            pltpu.VMEM((WIDTH, COLS * ROWS), BF16),
            pltpu.VMEM((WIDTH, COLS * ROWS), F32),
            pltpu.VMEM((WIDTH * S, ROWS), F32),
            pltpu.VMEM((2, CORES, 4, GROUP, WIDTH), BF16),
            pltpu.VMEM((WIDTH, WIDTH), BF16),
            pltpu.VMEM((WIDTH, WIDTH), BF16),
            pltpu.VMEM((WIDTH, WIDTH), F32),
            pltpu.VMEM((WIDTH, WIDTH), F32),
            pltpu.VMEM((2, PEERS, 2, COLS, ROWS), BF16),
            pltpu.VMEM((2, 2, 2, LINES, LINES), BF16),
            pltpu.VMEM((2, 2, REACH * BAND, LINES), BF16),
            pltpu.VMEM((WIDTH, COLS, ROWS), BF16),
            pltpu.SemaphoreType.DMA((9,)),
            pltpu.SemaphoreType.REGULAR,
            pltpu.SemaphoreType.REGULAR,
            pltpu.SemaphoreType.DMA((2,)),
            pltpu.SemaphoreType.DMA((2, 2)),
            pltpu.SemaphoreType.DMA((2, 2)),
            pltpu.SemaphoreType.DMA((2, 2)),
            pltpu.SemaphoreType.DMA((1 + len(PIECES),)),
            pltpu.SemaphoreType.DMA((1 + len(PIECES),)),
        ],
        compiler_params=pltpu.CompilerParams(
            collective_id=0, has_side_effects=True, vmem_limit_bytes=48_000_000
        ),
        name="triangle",
    )(*operands)


def solution(mesh):
    placed = (P(("unit", "north"), "east", None), P()) + (P("unit", None),) * 4
    placed += (P(),) + (P("unit", None),) * 2
    return jax.shard_map(
        body,
        mesh=mesh,
        in_specs=placed,
        out_specs=P(("unit", "north"), "east", None),
        check_vma=False,
    )
```
